128 devices in a mesh: seq: 32 (over x, z, core), tp: 4 (over y).
Axes of the slice: x: 4, y: 4, z: 4, core: 2. Of those that a mesh axis runs over, the one named last changes fastest.
Arguments:
- tokens: bfloat16 [65536, 2560], P('seq'), may hold values from -6 to 6
- w_query: bfloat16 [2560, 512], P(None, 'tp'), may hold values from -0.009765625 to 0.009765625
- w_key: bfloat16 [2560, 512], P(None, 'tp'), may hold values from -0.00048828125 to 0.00048828125
- w_value: bfloat16 [2560, 1024], P(None, 'tp'), may hold values from -0.125 to 0.125
- w_gate: bfloat16 [2560, 512], P(None, 'tp'), may hold values from -0.125 to 0.125
- gate_rate: float32 [512], P('tp'), may hold values from 3.8146973e-06 to 3.0517578e-05
- out_grad: bfloat16 [65536, 1024], P('seq', 'tp'), may hold values from -6 to 6
Outputs:
- input_grad: bfloat16 [65536, 2560], P(('seq', 'tp'))
- gate_signal: float32 [65536, 512], P('seq', 'tp')
The draws below stay inside these ranges and needn't reach their ends.
All inputs are finite; a program needn't handle non-finite values.
Results may differ from the reference program's by a relative error of at most 0.015.
Values sent between devices are 32-bit elements.
A program may use at most 192 MiB of HBM per device.

```python
import math
import jax
import jax.numpy as jnp
from jax import lax

D = 2560
DK = 128
DV = 256
CH = 128
HEADS = 4
TOKENS = 65536


def block_levels(stream_key, extent, split, smallest, high):
    def one(dim, shards_of):
        heights = jax.random.uniform(jax.random.fold_in(jax.random.fold_in(stream_key, 6), dim), (shards_of,), jnp.float32, smallest / len(split), high / len(split))
        return jnp.repeat(jnp.exp(heights), extent[dim] // shards_of).reshape((-1,) + (1,) * (len(extent) - dim - 1))

    gain = one(*split[0])
    for cut in split[1:]:
        gain = gain * one(*cut)
    return gain


def centred(own_key, shape, scale, limit, shards=(), dtype=jnp.bfloat16):
    drawn = scale * jax.random.normal(own_key, shape, jnp.float32)
    if shards:
        drawn = drawn * block_levels(own_key, shape, shards, -0.22, 0.18)
    return jnp.clip(drawn, -limit, limit).astype(dtype)


def setup_inputs(seed: int = 0) -> dict:
    seeds = jax.random.split(jax.random.key(seed), 8)
    return {
        "tokens": centred(seeds[0], (TOKENS, D), 1.0, 6.0, ((0, 32),)),
        "w_query": centred(seeds[1], (D, HEADS * DK), (D * DK) ** -0.5, 0.009765625, ((1, 4),)),
        "w_key": centred(seeds[2], (D, HEADS * DK), (D * TOKENS) ** -0.5, 0.00048828125, ((1, 4),)),
        "w_value": centred(seeds[3], (D, HEADS * DV), D ** -0.5, 0.125, ((1, 4),)),
        "w_gate": centred(seeds[4], (D, HEADS * DK), D ** -0.5, 0.125, ((1, 4),)),
        "gate_rate": jnp.clip(jnp.exp(math.log(3.0517578125e-05) - 2.0794415 * jax.random.uniform(seeds[5], (HEADS * DK,), jnp.float32) ** block_levels(seeds[5], (HEADS * DK,), ((0, 4),), -0.2, 0.2)), 3.814697265625e-06, 3.0517578125e-05),
        "out_grad": centred(seeds[6], (TOKENS, HEADS * DV), 1.0, 6.0, ((0, 32), (1, 4))),
    }


def lower_ones(length):
    places = jnp.arange(length)
    return (places[:, None] >= places[None, :]).astype(jnp.float32)

def low_dot(left, right):
    return jnp.dot(left.astype(jnp.bfloat16), right.astype(jnp.bfloat16), preferred_element_type=jnp.float32)

def run_head(query_rows, key_rows, value_rows, log_gate, initial):
    block_size = CH
    blocks_count = query_rows.shape[0] // block_size
    triangle = lower_ones(block_size)
    pieces = tuple((a.reshape(blocks_count, block_size, a.shape[1]) for a in (query_rows, key_rows, value_rows, log_gate)))

    def advance(memory, piece):
        query_block, key_block, value_block, gate_block = piece
        within = jnp.cumsum(gate_block, axis=0)
        closing = within[-1]
        query_scaled = query_block * jnp.exp(within)
        key_scaled = key_block * jnp.exp(-within)
        scores = low_dot(query_scaled, key_scaled.T) * triangle
        output = low_dot(query_scaled, memory) + low_dot(scores, value_block)
        key_closing = key_block * jnp.exp(closing - within)
        memory = jnp.exp(closing)[:, None] * memory + low_dot(key_closing.T, value_block)
        return (memory, output)
    last_memory, outputs = lax.scan(advance, initial, pieces)
    return (outputs.reshape(-1, outputs.shape[2]), last_memory)

def by_heads(matrix, width):
    return matrix.astype(jnp.float32).reshape(matrix.shape[0], -1, width).transpose(1, 0, 2)

def by_tokens(stacked):
    return stacked.transpose(1, 0, 2).reshape(stacked.shape[1], -1)

def back_project(grad_rows, weight):
    return lax.dot_general(grad_rows, weight, (((1,), (1,)), ((), ())), preferred_element_type=jnp.float32)

def reference(tokens, w_query, w_key, w_value, w_gate, gate_rate, out_grad):
    queries = jnp.dot(tokens, w_query, preferred_element_type=jnp.float32).astype(jnp.bfloat16)
    keys_proj = jnp.dot(tokens, w_key, preferred_element_type=jnp.float32).astype(jnp.bfloat16)
    values_proj = jnp.dot(tokens, w_value, preferred_element_type=jnp.float32).astype(jnp.bfloat16)
    squashed = jax.nn.sigmoid(jnp.dot(tokens, w_gate, preferred_element_type=jnp.float32))
    log_gate = -gate_rate * squashed
    initial = jnp.zeros((HEADS, DK, DV), jnp.float32)

    def forward(query_heads, key_heads, value_heads, gate_heads):
        outputs, last_memory = jax.vmap(run_head)(query_heads, key_heads, value_heads, gate_heads, initial)
        return outputs
    outputs, pullback = jax.vjp(forward, by_heads(queries, DK), by_heads(keys_proj, DK), by_heads(values_proj, DV), by_heads(log_gate, DK))
    grads = pullback(by_heads(out_grad, DV))
    query_grad = by_tokens(grads[0]).astype(jnp.bfloat16)
    key_grad = by_tokens(grads[1]).astype(jnp.bfloat16)
    value_grad = by_tokens(grads[2]).astype(jnp.bfloat16)
    pre_grad = by_tokens(grads[3]) * -gate_rate * squashed * (1.0 - squashed)
    gate_signal = pre_grad * (4.0 * math.sqrt(TOKENS * DK / DV))
    gate_grad = pre_grad.astype(jnp.bfloat16)
    mixed = back_project(query_grad, w_query) + back_project(key_grad, w_key)
    mixed = mixed + back_project(value_grad, w_value) + back_project(gate_grad, w_gate)
    return (mixed.astype(jnp.bfloat16), gate_signal)
```

```python
import functools
import math

import jax
import jax.numpy as jnp
from jax import lax
from jax.experimental import pallas as pl
from jax.experimental.pallas import tpu as pltpu
from jax.sharding import Mesh
from jax.sharding import PartitionSpec as P

DK = 128
DV = 256
BT = 256
NW = 3 * DK + DV
SEQ = ("seq_0", "seq_1", "seq_2")
SEQ_TP = ("seq_0", "seq_1", "seq_2", "tp")
MESH = pl.DeviceIdType.MESH
F32 = jnp.float32
BF16 = jnp.bfloat16


def mm(a, b):
    return lax.dot_general(a, b, (((1,), (0,)), ((), ())), preferred_element_type=F32)


def mm_nt(a, b):
    return lax.dot_general(a, b, (((1,), (1,)), ((), ())), preferred_element_type=F32)


def mm_tn(a, b):
    return lax.dot_general(a, b, (((0,), (0,)), ((), ())), preferred_element_type=F32)


def split(a):
    high = a.astype(BF16)
    return high, (a - high.astype(F32)).astype(BF16)


def body(dims, signal_scale, tok_hbm, wq, wk, wv, wg, rate_ref, og_hbm, gs_hbm, all_hbm,
         w_s, tok_s, og_s, qt, kt, vs, cs, sq, tri, carry, spre, gpre, dmsg, dpart, zsend, zrecv, zexc,
         xsend, xrecv, fsend, frecv, psend, states, gbuf, rbuf, gsb, allb,
         load_sem, tok_sem, d_sem, z_sem, x_sem, f_sem, p_sem, a_sem, out_sem):
    nx, nz, ny, rows, width, blocks = dims
    x, z, c, y = (lax.axis_index(a) for a in SEQ_TP)
    sgn = 1 - 2 * c
    per_chunk = blocks // ny
    quarter = DV // nz
    pairs = blocks // 2

    barrier = pltpu.get_barrier_semaphore()
    xrecv[...] = jnp.zeros_like(xrecv)
    peers = [{"seq_2": 1 - c}]
    peers += [{"seq_0": lax.rem(x + d, nx)} for d in range(1, nx)]
    peers += [{"seq_1": lax.rem(z + d, nz)} for d in range(1, nz)]
    peers += [{"tp": lax.rem(y + d, ny)} for d in range(1, ny)]
    for peer in peers:
        pl.semaphore_signal(barrier, inc=1, device_id=peer, device_id_type=MESH)

    loads = [
        pltpu.make_async_copy(wq, w_s.at[:, pl.ds(0, DK)], load_sem.at[0]),
        pltpu.make_async_copy(wk, w_s.at[:, pl.ds(DK, DK)], load_sem.at[1]),
        pltpu.make_async_copy(wv, w_s.at[:, pl.ds(2 * DK, DV)], load_sem.at[2]),
        pltpu.make_async_copy(wg, w_s.at[:, pl.ds(2 * DK + DV, DK)], load_sem.at[3]),
        pltpu.make_async_copy(og_hbm, og_s, load_sem.at[4]),
    ]

    def tok_copy(i):
        slot = lax.rem(i, 2)
        start = pl.multiple_of(i * 2 * BT, 2 * BT)
        return pltpu.make_async_copy(tok_hbm.at[pl.ds(start, 2 * BT)], tok_s.at[slot], tok_sem.at[slot])

    tok_copy(0).start()
    for load in loads:
        load.start()

    at = lax.broadcasted_iota(jnp.int32, (BT, BT), 0)
    before = lax.broadcasted_iota(jnp.int32, (BT, BT), 1)
    tri[0] = (at >= before).astype(F32).astype(BF16)
    tri[1] = (at <= before).astype(F32).astype(BF16)
    carry[...] = jnp.zeros_like(carry)
    spre[0] = jnp.zeros((DV, DK), F32)
    gpre[0] = jnp.zeros((DV, DK), F32)
    rate = rate_ref[...]
    for load in loads:
        load.wait()

    @pl.loop(0, pairs)
    def _(i):
        slot = lax.rem(i, 2)

        @pl.when(i + 1 < pairs)
        def _():
            tok_copy(i + 1).start()

        tok_copy(i).wait()
        here = tok_s[slot]
        qk = mm(here, w_s[:, 0:2 * DK])
        val = mm(here, w_s[:, 2 * DK:2 * DK + DV])
        gate = mm(here, w_s[:, 2 * DK + DV:])
        for half in range(2):
            b = i * 2 + half
            at_rows = pl.ds(pl.multiple_of(b * BT, BT), BT)
            part = slice(half * BT, (half + 1) * BT)
            squashed = jax.nn.sigmoid(gate[part])
            sq[at_rows, :] = squashed
            high, low = split(-rate * squashed)
            running = mm(tri[0], high) + mm(tri[0], low) + carry[0:1, :]
            carry[0:1, :] = running[BT - 1:BT, :]
            cs[at_rows, :] = running
            q_here = qk[part, 0:DK].astype(BF16).astype(F32)
            k_here = qk[part, DK:2 * DK].astype(BF16).astype(F32)
            q_run = (q_here * jnp.exp(running)).astype(BF16)
            k_run = (k_here * jnp.exp(-running)).astype(BF16)
            v_here = val[part].astype(BF16)
            qt[at_rows, :] = q_run
            kt[at_rows, :] = k_run
            vs[at_rows, :] = v_here
            spre[b + 1] = spre[b] + mm_tn(v_here, k_run)
            gpre[b + 1] = gpre[b] + mm_tn(og_s[at_rows, :], q_run)

    log_total = carry[0:1, :]
    decay = jnp.exp(log_total)
    dmsg[0, 0:DV, :] = spre[blocks] * decay
    dmsg[1, 0:DV, :] = gpre[blocks]
    for kind in range(2):
        dmsg[kind, DV:DV + 8, :] = jnp.broadcast_to(log_total, (8, DK))
    pl.semaphore_wait(barrier, len(peers))

    d_copy = pltpu.make_async_remote_copy(
        dmsg.at[1 - c], dpart, d_sem.at[0], d_sem.at[1], device_id={"seq_2": 1 - c}, device_id_type=MESH)
    d_copy.start()
    d_copy.wait()
    chip_log = log_total + dpart[DV:DV + 1, :]
    chip = dpart[0:DV, :] + jnp.exp(dpart[DV:DV + 1, :]) * dmsg[c, 0:DV, :]
    for n in range(nz):
        zsend[n, 0:quarter, :] = chip[n * quarter:(n + 1) * quarter, :]
        zsend[n, quarter:quarter + 8, :] = jnp.broadcast_to(chip_log, (8, DK))
    zrecv[z] = zsend[z]
    z_copies = []
    for d in range(1, nz):
        to = lax.rem(z + d, nz)
        z_copies.append(pltpu.make_async_remote_copy(
            zsend.at[to], zrecv.at[z], z_sem.at[0, d - 1], z_sem.at[1, d - 1],
            device_id={"seq_1": to}, device_id_type=MESH))
    for copy in z_copies:
        copy.start()
    for copy in z_copies:
        copy.wait()
    total = jnp.zeros((quarter, DK), F32)
    total_log = jnp.zeros((1, DK), F32)
    for n in range(nz):
        src = c * (nz - 1) + sgn * n
        zexc[src, 0:quarter, :] = total
        zexc[src, quarter:quarter + 8, :] = jnp.broadcast_to(total_log, (8, DK))
        log_here = zrecv[src, quarter:quarter + 1, :]
        total = zrecv[src, 0:quarter, :] + jnp.exp(log_here) * total
        total_log = total_log + log_here
    xsend[0:quarter, :] = total
    xsend[quarter:quarter + 8, :] = jnp.broadcast_to(total_log, (8, DK))

    def x_copy(d):
        to = x + sgn * d
        inside = (to >= 0) & (to < nx)
        return inside, pltpu.make_async_remote_copy(
            xsend, xrecv.at[d - 1], x_sem.at[0, d - 1], x_sem.at[1, d - 1],
            device_id={"seq_0": jnp.where(inside, to, 1 - jnp.minimum(x, 1))}, device_id_type=MESH)

    for d in range(1, nx):
        inside, copy = x_copy(d)
        pl.when(inside)(copy.start)
    for d in range(1, nx):
        inside, copy = x_copy(d)
        pl.when(inside)(copy.wait_send)
        source = x - sgn * d
        pl.when((source >= 0) & (source < nx))(copy.wait_recv)
    entering = jnp.zeros((quarter, DK), F32)
    for d in reversed(range(1, nx)):
        entering = xrecv[d - 1, 0:quarter, :] + jnp.exp(xrecv[d - 1, quarter:quarter + 1, :]) * entering
    for n in range(nz):
        fsend[n] = zexc[n, 0:quarter, :] + jnp.exp(zexc[n, quarter:quarter + 1, :]) * entering
    frecv[z] = fsend[z]
    f_copies = []
    for d in range(1, nz):
        to = lax.rem(z + d, nz)
        f_copies.append(pltpu.make_async_remote_copy(
            fsend.at[to], frecv.at[z], f_sem.at[0, d - 1], f_sem.at[1, d - 1],
            device_id={"seq_1": to}, device_id_type=MESH))
    for copy in f_copies:
        copy.start()
    for copy in f_copies:
        copy.wait()
    entered = frecv[...].reshape(DV, DK)
    psend[...] = dmsg[c, 0:DV, :] + decay * entered
    states[c] = entered
    p_copy = pltpu.make_async_remote_copy(
        psend, states.at[c], p_sem.at[0], p_sem.at[1], device_id={"seq_2": 1 - c}, device_id_type=MESH)
    p_copy.start()
    p_copy.wait()
    states[1] = states[1] * decay

    def a_copy(n):
        o = lax.rem(n // per_chunk + 1, ny)
        i = lax.rem(n, per_chunk)
        to = lax.rem(y + o, ny)
        b = to * per_chunk + i
        return o, i, to, b

    def start_send(n):
        o, i, to, b = a_copy(n)
        dst = pl.ds(pl.multiple_of(i * BT, BT), BT)
        slot = o - 1
        return pltpu.make_async_remote_copy(
            gbuf.at[b], rbuf.at[slot, dst], a_sem.at[0, slot, i], a_sem.at[1, slot, i],
            device_id={"tp": to}, device_id_type=MESH)

    remote = blocks - per_chunk

    @pl.loop(0, blocks)
    def _(n):
        o, i, to, b = a_copy(n)
        at_rows = pl.ds(pl.multiple_of(b * BT, BT), BT)
        q_run = qt[at_rows, :]
        k_run = kt[at_rows, :]
        v_here = vs[at_rows, :]
        o_grad = og_s[at_rows, :]
        running = cs[at_rows, :]
        squashed = sq[at_rows, :]
        upper = tri[1].astype(F32)
        lower = tri[0].astype(F32)
        scores_t = (mm_nt(k_run, q_run) * upper).astype(BF16)
        d_scores = (mm_nt(o_grad, v_here) * lower).astype(BF16)
        d_scores_t = (mm_nt(v_here, o_grad) * upper).astype(BF16)
        state = states[0] + spre[b]
        after = states[0] + spre[b + 1]
        cotangent = states[1] + (gpre[blocks] - gpre[b + 1])
        state_low = state.astype(BF16)
        cot_low = cotangent.astype(BF16)
        dv = mm(scores_t, o_grad) + mm_nt(k_run, cot_low)
        dq = mm(o_grad, state_low) + mm(d_scores, k_run)
        dk = mm(v_here, cot_low) + mm(d_scores_t, q_run)
        boundary = jnp.sum(after * cotangent, axis=0, keepdims=True)
        high, low = split(q_run.astype(F32) * dq - k_run.astype(F32) * dk)
        dg = mm(tri[1], high) + mm(tri[1], low) + boundary
        pre = dg * (-rate) * squashed * (1.0 - squashed)
        gsb[at_rows, :] = pre * signal_scale
        gbuf[b, :, 0:DK] = dq * jnp.exp(running)
        gbuf[b, :, DK:2 * DK] = dk * jnp.exp(-running)
        gbuf[b, :, 2 * DK:2 * DK + DV] = dv
        gbuf[b, :, 2 * DK + DV:] = pre

        @pl.when((n >= 1) & (n - 1 < remote))
        def _():
            start_send(n - 1).start()

    gs_copy = pltpu.make_async_copy(gsb, gs_hbm, out_sem.at[0])
    gs_copy.start()
    for i in range(per_chunk):
        allb[i * BT:(i + 1) * BT, pl.ds(pl.multiple_of(y * NW, 128), NW)] = gbuf[y * per_chunk + i].astype(BF16)

    @pl.loop(0, remote)
    def _(n):
        copy = start_send(n)
        copy.wait_send()
        copy.wait_recv()

    for o in range(1, ny):
        head = lax.rem(y - o + ny, ny)
        allb[:, pl.ds(pl.multiple_of(head * NW, 128), NW)] = rbuf[o - 1].astype(BF16)
    all_copy = pltpu.make_async_copy(allb, all_hbm, out_sem.at[1])
    all_copy.start()
    all_copy.wait()
    gs_copy.wait()


def mix_body(g_ref, w_ref, o_ref):
    heads = w_ref.shape[0]
    total = None
    for h in range(heads):
        term = mm_nt(g_ref[:, h * NW:(h + 1) * NW], w_ref[h].astype(BF16))
        total = term if total is None else total + term
    o_ref[...] = total.astype(BF16)


def per_device(dims, tokens, w_query, w_key, w_value, w_gate, gate_rate, out_grad):
    nx, nz, ny = dims
    rows, width = tokens.shape
    blocks = rows // BT
    mine = rows // ny
    quarter = DV // nz
    whole_tokens = rows * nx * nz * 2
    signal_scale = 4.0 * math.sqrt(whole_tokens * DK / DV)

    spot = (lax.axis_index("seq_0") * nz + lax.axis_index("seq_1")) * 2 + lax.axis_index("seq_2")
    share = width // (nx * nz * 2)
    pieces = [lax.dynamic_slice_in_dim(w, spot * share, share, 0) for w in (w_query, w_key, w_value, w_gate)]
    piece = jnp.concatenate(pieces, axis=1).astype(F32)
    gathered = lax.all_gather(piece, "tp")
    gathered = lax.all_gather(gathered, SEQ, axis=1, tiled=True)

    any_spec = pl.BlockSpec(memory_space=pl.ANY)
    vmem_spec = pl.BlockSpec(memory_space=pltpu.VMEM)
    dma = pltpu.SemaphoreType.DMA
    signal, grads = pl.pallas_call(
        functools.partial(body, (nx, nz, ny, rows, width, blocks), signal_scale),
        out_shape=(
            jax.ShapeDtypeStruct((rows, DK), F32),
            jax.ShapeDtypeStruct((mine, ny * NW), BF16),
        ),
        in_specs=[any_spec] * 5 + [vmem_spec, any_spec],
        out_specs=(any_spec, any_spec),
        scratch_shapes=[
            pltpu.VMEM((width, NW), BF16),
            pltpu.VMEM((2, 2 * BT, width), BF16),
            pltpu.VMEM((rows, DV), BF16),
            pltpu.VMEM((rows, DK), BF16),
            pltpu.VMEM((rows, DK), BF16),
            pltpu.VMEM((rows, DV), BF16),
            pltpu.VMEM((rows, DK), F32),
            pltpu.VMEM((rows, DK), F32),
            pltpu.VMEM((2, BT, BT), BF16),
            pltpu.VMEM((8, DK), F32),
            pltpu.VMEM((blocks + 1, DV, DK), F32),
            pltpu.VMEM((blocks + 1, DV, DK), F32),
            pltpu.VMEM((2, DV + 8, DK), F32),
            pltpu.VMEM((DV + 8, DK), F32),
            pltpu.VMEM((nz, quarter + 8, DK), F32),
            pltpu.VMEM((nz, quarter + 8, DK), F32),
            pltpu.VMEM((nz, quarter + 8, DK), F32),
            pltpu.VMEM((quarter + 8, DK), F32),
            pltpu.VMEM((nx - 1, quarter + 8, DK), F32),
            pltpu.VMEM((nz, quarter, DK), F32),
            pltpu.VMEM((nz, quarter, DK), F32),
            pltpu.VMEM((DV, DK), F32),
            pltpu.VMEM((2, DV, DK), F32),
            pltpu.VMEM((blocks, BT, NW), F32),
            pltpu.VMEM((ny - 1, mine, NW), F32),
            pltpu.VMEM((rows, DK), F32),
            pltpu.VMEM((mine, ny * NW), BF16),
            dma((5,)),
            dma((2,)),
            dma((2,)),
            dma((2, nz - 1)),
            dma((2, nx - 1)),
            dma((2, nz - 1)),
            dma((2,)),
            dma((2, ny - 1, blocks // ny)),
            dma((2,)),
        ],
        compiler_params=pltpu.CompilerParams(
            collective_id=0, has_side_effects=True, vmem_limit_bytes=60 * 2**20),
        cost_estimate=pl.CostEstimate(
            flops=40_000_000_000, bytes_accessed=30_000_000, transcendentals=1_000_000),
    )(tokens, w_query, w_key, w_value, w_gate, gate_rate.reshape(1, DK), out_grad)

    tile = 128
    mixed = pl.pallas_call(
        mix_body,
        grid=(width // tile,),
        out_shape=jax.ShapeDtypeStruct((mine, width), BF16),
        in_specs=[
            pl.BlockSpec((mine, ny * NW), lambda i: (0, 0)),
            pl.BlockSpec((ny, tile, NW), lambda i: (0, i, 0)),
        ],
        out_specs=pl.BlockSpec((mine, tile), lambda i: (0, i)),
    )(grads, gathered)
    return mixed, signal


def solution(mesh, shape=(4, 4)):
    nx, nz = shape
    ny = mesh.shape["tp"]
    torus = Mesh(mesh.devices.reshape(nx, nz, 2, ny), SEQ_TP)
    placed = (
        P(SEQ, None),
        P(None, "tp"),
        P(None, "tp"),
        P(None, "tp"),
        P(None, "tp"),
        P("tp"),
        P(SEQ, "tp"),
    )
    return jax.shard_map(
        functools.partial(per_device, (nx, nz, ny)),
        mesh=torus,
        in_specs=placed,
        out_specs=(P(SEQ_TP, None), P(SEQ, "tp")),
        check_vma=False,
    )
```

```python
import functools
import math

import jax
import jax.numpy as jnp
from jax import lax
from jax.experimental import pallas as pl
from jax.experimental.pallas import tpu as pltpu
from jax.sharding import Mesh
from jax.sharding import PartitionSpec as P

DK = 128
DV = 256
BT = 256
NW = 3 * DK + DV
SEQ = ("seq_0", "seq_1", "seq_2")
SEQ_TP = ("seq_0", "seq_1", "seq_2", "tp")
MESH = pl.DeviceIdType.MESH
F32 = jnp.float32
BF16 = jnp.bfloat16


def mm(a, b):
    return lax.dot_general(a, b, (((1,), (0,)), ((), ())), preferred_element_type=F32)


def mm_nt(a, b):
    return lax.dot_general(a, b, (((1,), (1,)), ((), ())), preferred_element_type=F32)


def mm_tn(a, b):
    return lax.dot_general(a, b, (((0,), (0,)), ((), ())), preferred_element_type=F32)


def split(a):
    high = a.astype(BF16)
    return high, (a - high.astype(F32)).astype(BF16)


def body(dims, signal_scale, tok_hbm, wq, wk, wv, wg, rate_ref, og_hbm, out_hbm, gs_hbm,
         w_s, tok_s, og_s, qt, kt, vs, cs, sq, tri, carry, spre, gpre, dmsg, dpart, zsend, zrecv, zexc,
         xsend, xrecv, fsend, frecv, psend, states, gbuf, rbuf, gsb, acc, wsend, wl,
         load_sem, tok_sem, d_sem, z_sem, x_sem, f_sem, p_sem, a_sem, out_sem,
         wy_sem, w1_sem, f1_sem, w2_sem, f2_sem, wd_sem):
    nx, nz, ny, rows, width, blocks = dims
    x, z, c, y = (lax.axis_index(a) for a in SEQ_TP)
    sgn = 1 - 2 * c
    per_chunk = blocks // ny
    quarter = DV // nz
    pairs = blocks // 2
    mine = rows // ny

    ring = nx
    share = width // (ring * ring * 2)
    first = x + c * (z - x)
    second = z + c * (x - z)

    def place(a, b):
        return {"seq_0": a + c * (b - a), "seq_1": b + c * (a - b)}

    def wrap(v):
        return lax.rem(v + ring, ring)

    def share_at(a, b, part, parts):
        size = share // parts
        start = ((c * ring + a) * ring + b) * share + part * size
        return pl.ds(pl.multiple_of(start, 8), size)

    def group_at(a, part, parts):
        size = ring * share // parts
        start = (c * ring + a) * ring * share + part * size
        return pl.ds(pl.multiple_of(start, 8), size)

    def remote(src, dst, sems, i, to):
        return pltpu.make_async_remote_copy(
            src, dst, sems.at[(0, *i)], sems.at[(1, *i)], device_id=to, device_id_type=MESH)

    def wy_copy(o):
        dst = wl.at[o - 1, share_at(first, second, 0, 1)]
        return remote(wsend, dst, wy_sem, (o - 1,), {"tp": lax.rem(y + o, ny)})

    turns = (0, 1) if ring > 2 else (0,)

    def w1_copy(s, turn):
        ref = wl.at[s, share_at(first, second, 0, 1)]
        return remote(ref, ref, w1_sem, (s, turn), place(first, wrap(second + 1 - 2 * turn)))

    def f1_copy(s, turn):
        ref = wl.at[s, share_at(first, wrap(second - 1 + 2 * turn), turn, 2)]
        return remote(ref, ref, f1_sem, (s, turn), place(first, wrap(second + 1 - 2 * turn)))

    def w2_copy(s, turn):
        ref = wl.at[s, group_at(first, 0, 1)]
        return remote(ref, ref, w2_sem, (s, turn), place(wrap(first + 1 - 2 * turn), second))

    def f2_copy(s, turn):
        ref = wl.at[s, group_at(wrap(first - 1 + 2 * turn), turn, 2)]
        return remote(ref, ref, f2_sem, (s, turn), place(wrap(first + 1 - 2 * turn), second))

    def wd_copy(s, n):
        ref = wl.at[s, group_at(lax.rem(first + n, ring), 0, 1)]
        return remote(ref, ref, wd_sem, (s, n), {"seq_2": 1 - c})

    def start_all(copy, s):
        for turn in turns:
            copy(s, turn).start()

    def arrive_all(copy, s):
        for turn in turns:
            copy(s, turn).wait_recv()

    barrier = pltpu.get_barrier_semaphore()
    xrecv[...] = jnp.zeros_like(xrecv)
    peers = [{"seq_2": 1 - c}]
    peers += [{"seq_0": lax.rem(x + d, nx)} for d in range(1, nx)]
    peers += [{"seq_1": lax.rem(z + d, nz)} for d in range(1, nz)]
    peers += [{"tp": lax.rem(y + d, ny)} for d in range(1, ny)]
    for peer in peers:
        pl.semaphore_signal(barrier, inc=1, device_id=peer, device_id_type=MESH)

    loads = [
        pltpu.make_async_copy(wq, w_s.at[:, pl.ds(0, DK)], load_sem.at[0]),
        pltpu.make_async_copy(wk, w_s.at[:, pl.ds(DK, DK)], load_sem.at[1]),
        pltpu.make_async_copy(wv, w_s.at[:, pl.ds(2 * DK, DV)], load_sem.at[2]),
        pltpu.make_async_copy(wg, w_s.at[:, pl.ds(2 * DK + DV, DK)], load_sem.at[3]),
        pltpu.make_async_copy(og_hbm, og_s, load_sem.at[4]),
    ]

    def tok_copy(i):
        slot = lax.rem(i, 2)
        start = pl.multiple_of(i * 2 * BT, 2 * BT)
        return pltpu.make_async_copy(tok_hbm.at[pl.ds(start, 2 * BT)], tok_s.at[slot], tok_sem.at[slot])

    tok_copy(0).start()
    for load in loads:
        load.start()

    at = lax.broadcasted_iota(jnp.int32, (BT, BT), 0)
    before = lax.broadcasted_iota(jnp.int32, (BT, BT), 1)
    tri[0] = (at >= before).astype(F32).astype(BF16)
    tri[1] = (at <= before).astype(F32).astype(BF16)
    carry[...] = jnp.zeros_like(carry)
    spre[0] = jnp.zeros((DV, DK), F32)
    gpre[0] = jnp.zeros((DV, DK), F32)
    rate = rate_ref[...]
    for load in loads:
        load.wait()
    wsend[...] = w_s[share_at(first, second, 0, 1), :].astype(F32)
    pl.semaphore_wait(barrier, len(peers))
    for o in range(1, ny):
        wy_copy(o).start()

    with jax.named_scope("proj"):
        @pl.loop(0, pairs)
        def _(i):
            slot = lax.rem(i, 2)

            @pl.when(i + 1 < pairs)
            def _():
                tok_copy(i + 1).start()

            tok_copy(i).wait()
            here = tok_s[slot]
            qk = mm(here, w_s[:, 0:2 * DK])
            val = mm(here, w_s[:, 2 * DK:2 * DK + DV])
            gate = mm(here, w_s[:, 2 * DK + DV:])
            for half in range(2):
                b = i * 2 + half
                at_rows = pl.ds(pl.multiple_of(b * BT, BT), BT)
                part = slice(half * BT, (half + 1) * BT)
                squashed = jax.nn.sigmoid(gate[part])
                sq[at_rows, :] = squashed
                high, low = split(-rate * squashed)
                running = mm(tri[0], high) + mm(tri[0], low) + carry[0:1, :]
                carry[0:1, :] = running[BT - 1:BT, :]
                cs[at_rows, :] = running
                q_here = qk[part, 0:DK].astype(BF16).astype(F32)
                k_here = qk[part, DK:2 * DK].astype(BF16).astype(F32)
                q_run = (q_here * jnp.exp(running)).astype(BF16)
                k_run = (k_here * jnp.exp(-running)).astype(BF16)
                v_here = val[part].astype(BF16)
                qt[at_rows, :] = q_run
                kt[at_rows, :] = k_run
                vs[at_rows, :] = v_here
                spre[b + 1] = spre[b] + mm_tn(v_here, k_run)
                gpre[b + 1] = gpre[b] + mm_tn(og_s[at_rows, :], q_run)


    log_total = carry[0:1, :]
    decay = jnp.exp(log_total)
    dmsg[0, 0:DV, :] = spre[blocks] * decay
    dmsg[1, 0:DV, :] = gpre[blocks]
    for kind in range(2):
        dmsg[kind, DV:DV + 8, :] = jnp.broadcast_to(log_total, (8, DK))

    d_copy = pltpu.make_async_remote_copy(
        dmsg.at[1 - c], dpart, d_sem.at[0], d_sem.at[1], device_id={"seq_2": 1 - c}, device_id_type=MESH)
    with jax.named_scope("d2d"):
        d_copy.start()
        d_copy.wait()

    chip_log = log_total + dpart[DV:DV + 1, :]
    chip = dpart[0:DV, :] + jnp.exp(dpart[DV:DV + 1, :]) * dmsg[c, 0:DV, :]
    for n in range(nz):
        zsend[n, 0:quarter, :] = chip[n * quarter:(n + 1) * quarter, :]
        zsend[n, quarter:quarter + 8, :] = jnp.broadcast_to(chip_log, (8, DK))
    zrecv[z] = zsend[z]
    z_copies = []
    for d in range(1, nz):
        to = lax.rem(z + d, nz)
        z_copies.append(pltpu.make_async_remote_copy(
            zsend.at[to], zrecv.at[z], z_sem.at[0, d - 1], z_sem.at[1, d - 1],
            device_id={"seq_1": to}, device_id_type=MESH))
    for copy in z_copies:
        copy.start()
    slots = [0, 2, 1][: ny - 1] if ny > 2 else [0]
    for s in range(ny - 1):
        wy_copy(s + 1).wait_recv()
    start_all(w1_copy, slots[0])
    with jax.named_scope("zex"):
        for copy in z_copies:
            copy.wait()

    total = jnp.zeros((quarter, DK), F32)
    total_log = jnp.zeros((1, DK), F32)
    for n in range(nz):
        src = c * (nz - 1) + sgn * n
        zexc[src, 0:quarter, :] = total
        zexc[src, quarter:quarter + 8, :] = jnp.broadcast_to(total_log, (8, DK))
        log_here = zrecv[src, quarter:quarter + 1, :]
        total = zrecv[src, 0:quarter, :] + jnp.exp(log_here) * total
        total_log = total_log + log_here
    xsend[0:quarter, :] = total
    xsend[quarter:quarter + 8, :] = jnp.broadcast_to(total_log, (8, DK))

    def x_copy(d):
        to = x + sgn * d
        inside = (to >= 0) & (to < nx)
        return inside, pltpu.make_async_remote_copy(
            xsend, xrecv.at[d - 1], x_sem.at[0, d - 1], x_sem.at[1, d - 1],
            device_id={"seq_0": jnp.where(inside, to, 1 - jnp.minimum(x, 1))}, device_id_type=MESH)

    for d in range(1, nx):
        inside, copy = x_copy(d)
        pl.when(inside)(copy.start)
    for s in slots[1:2]:
        start_all(w1_copy, s)
    with jax.named_scope("xex"):
        for d in range(1, nx):
            inside, copy = x_copy(d)
            pl.when(inside)(copy.wait_send)
            source = x - sgn * d
            pl.when((source >= 0) & (source < nx))(copy.wait_recv)

    entering = jnp.zeros((quarter, DK), F32)
    for d in reversed(range(1, nx)):
        entering = xrecv[d - 1, 0:quarter, :] + jnp.exp(xrecv[d - 1, quarter:quarter + 1, :]) * entering
    for n in range(nz):
        fsend[n] = zexc[n, 0:quarter, :] + jnp.exp(zexc[n, quarter:quarter + 1, :]) * entering
    frecv[z] = fsend[z]
    f_copies = []
    for d in range(1, nz):
        to = lax.rem(z + d, nz)
        f_copies.append(pltpu.make_async_remote_copy(
            fsend.at[to], frecv.at[z], f_sem.at[0, d - 1], f_sem.at[1, d - 1],
            device_id={"seq_1": to}, device_id_type=MESH))
    for copy in f_copies:
        copy.start()
    for s in slots[2:]:
        start_all(w1_copy, s)
    with jax.named_scope("fex"):
        for copy in f_copies:
            copy.wait()

    entered = frecv[...].reshape(DV, DK)
    psend[...] = dmsg[c, 0:DV, :] + decay * entered
    states[c] = entered
    p_copy = pltpu.make_async_remote_copy(
        psend, states.at[c], p_sem.at[0], p_sem.at[1], device_id={"seq_2": 1 - c}, device_id_type=MESH)
    with jax.named_scope("pex"):
        p_copy.start()
        p_copy.wait()

    states[1] = states[1] * decay
    for s in slots:
        arrive_all(w1_copy, s)
        if ring > 2:
            start_all(f1_copy, s)

    def a_copy(n):
        o = lax.rem(n // per_chunk + 1, ny)
        i = lax.rem(n, per_chunk)
        to = lax.rem(y + o, ny)
        b = to * per_chunk + i
        return o, i, to, b

    def start_send(n):
        o, i, to, b = a_copy(n)
        dst = pl.ds(pl.multiple_of(i * BT, BT), BT)
        slot = o - 1
        return pltpu.make_async_remote_copy(
            gbuf.at[b], rbuf.at[slot, dst], a_sem.at[0, slot, i], a_sem.at[1, slot, i],
            device_id={"tp": to}, device_id_type=MESH)

    sent = blocks - per_chunk

    with jax.named_scope("blk"):
        @pl.loop(0, blocks)
        def _(n):
            o, i, to, b = a_copy(n)
            at_rows = pl.ds(pl.multiple_of(b * BT, BT), BT)
            q_run = qt[at_rows, :]
            k_run = kt[at_rows, :]
            v_here = vs[at_rows, :]
            o_grad = og_s[at_rows, :]
            running = cs[at_rows, :]
            squashed = sq[at_rows, :]
            upper = tri[1].astype(F32)
            lower = tri[0].astype(F32)
            scores_t = (mm_nt(k_run, q_run) * upper).astype(BF16)
            d_scores = (mm_nt(o_grad, v_here) * lower).astype(BF16)
            d_scores_t = (mm_nt(v_here, o_grad) * upper).astype(BF16)
            state = states[0] + spre[b]
            after = states[0] + spre[b + 1]
            cotangent = states[1] + (gpre[blocks] - gpre[b + 1])
            state_low = state.astype(BF16)
            cot_low = cotangent.astype(BF16)
            dv = mm(scores_t, o_grad) + mm_nt(k_run, cot_low)
            dq = mm(o_grad, state_low) + mm(d_scores, k_run)
            dk = mm(v_here, cot_low) + mm(d_scores_t, q_run)
            boundary = jnp.sum(after * cotangent, axis=0, keepdims=True)
            high, low = split(q_run.astype(F32) * dq - k_run.astype(F32) * dk)
            dg = mm(tri[1], high) + mm(tri[1], low) + boundary
            pre = dg * (-rate) * squashed * (1.0 - squashed)
            gsb[at_rows, :] = pre * signal_scale
            gbuf[b, :, 0:DK] = dq * jnp.exp(running)
            gbuf[b, :, DK:2 * DK] = dk * jnp.exp(-running)
            gbuf[b, :, 2 * DK:2 * DK + DV] = dv
            gbuf[b, :, 2 * DK + DV:] = pre

            @pl.when((n >= 1) & (n - 1 < sent))
            def _():
                start_send(n - 1).start()

            @pl.when(n == 2)
            def _():
                for s in slots:
                    if ring > 2:
                        arrive_all(f1_copy, s)
                    start_all(w2_copy, s)


    gs_copy = pltpu.make_async_copy(gsb, gs_hbm, out_sem.at[0])
    gs_copy.start()
    cols = min(512, width)

    def mix(grads, weights, last):
        @pl.loop(0, width // cols)
        def _(i):
            at = pl.ds(pl.multiple_of(i * cols, cols), cols)
            term = mm_nt(grads, weights(at))
            if last is None:
                acc[:, at] = term
            elif last:
                tok_s[0, 0:mine, at] = (acc[:, at] + term).astype(BF16)
            else:
                acc[:, at] = acc[:, at] + term

    with jax.named_scope("mix_own"):
        own = gbuf[pl.ds(y * per_chunk, per_chunk)].reshape(mine, NW).astype(BF16)
        mix(own, lambda at: w_s[at, :], None)
    with jax.named_scope("weights"):
        for s in slots:
            for n in range(1):
                wd_copy(s, n).start()
        for s in slots:
            arrive_all(w2_copy, s)
            if ring > 2:
                start_all(f2_copy, s)
            wd_copy(s, 1).start()
            if ring > 2:
                wd_copy(s, ring - 1).start()
        if ring > 2:
            for s in slots:
                arrive_all(f2_copy, s)
                wd_copy(s, 2).start()
        for s in slots:
            for n in range(ring):
                wd_copy(s, n).wait_recv()
    for s in slots:
        with jax.named_scope("grads"):
            for i in range(per_chunk):
                start_send(s * per_chunk + i).wait_recv()
        with jax.named_scope("mix"):
            mix(rbuf[s].astype(BF16), lambda at: wl[s, at, :].astype(BF16), s == slots[-1])
    out_copy = pltpu.make_async_copy(tok_s.at[0, pl.ds(0, mine)], out_hbm, out_sem.at[1])
    out_copy.start()
    for o in range(1, ny):
        wy_copy(o).wait_send()
    for s in slots:
        for turn in turns:
            w1_copy(s, turn).wait_send()
            w2_copy(s, turn).wait_send()
            if ring > 2:
                f1_copy(s, turn).wait_send()
                f2_copy(s, turn).wait_send()
        for n in range(ring):
            wd_copy(s, n).wait_send()

    @pl.loop(0, sent)
    def _(n):
        start_send(n).wait_send()

    out_copy.wait()
    gs_copy.wait()


def per_device(dims, tokens, w_query, w_key, w_value, w_gate, gate_rate, out_grad):
    nx, nz, ny = dims
    rows, width = tokens.shape
    blocks = rows // BT
    mine = rows // ny
    quarter = DV // nz
    whole_tokens = rows * nx * nz * 2
    signal_scale = 4.0 * math.sqrt(whole_tokens * DK / DV)

    any_spec = pl.BlockSpec(memory_space=pl.ANY)
    vmem_spec = pl.BlockSpec(memory_space=pltpu.VMEM)
    dma = pltpu.SemaphoreType.DMA
    mixed, signal = pl.pallas_call(
        functools.partial(body, (nx, nz, ny, rows, width, blocks), signal_scale),
        out_shape=(
            jax.ShapeDtypeStruct((mine, width), BF16),
            jax.ShapeDtypeStruct((rows, DK), F32),
        ),
        in_specs=[any_spec] * 5 + [vmem_spec, any_spec],
        out_specs=(any_spec, any_spec),
        scratch_shapes=[
            pltpu.VMEM((width, NW), BF16),
            pltpu.VMEM((2, 2 * BT, width), BF16),
            pltpu.VMEM((rows, DV), BF16),
            pltpu.VMEM((rows, DK), BF16),
            pltpu.VMEM((rows, DK), BF16),
            pltpu.VMEM((rows, DV), BF16),
            pltpu.VMEM((rows, DK), F32),
            pltpu.VMEM((rows, DK), F32),
            pltpu.VMEM((2, BT, BT), BF16),
            pltpu.VMEM((8, DK), F32),
            pltpu.VMEM((blocks + 1, DV, DK), F32),
            pltpu.VMEM((blocks + 1, DV, DK), F32),
            pltpu.VMEM((2, DV + 8, DK), F32),
            pltpu.VMEM((DV + 8, DK), F32),
            pltpu.VMEM((nz, quarter + 8, DK), F32),
            pltpu.VMEM((nz, quarter + 8, DK), F32),
            pltpu.VMEM((nz, quarter + 8, DK), F32),
            pltpu.VMEM((quarter + 8, DK), F32),
            pltpu.VMEM((nx - 1, quarter + 8, DK), F32),
            pltpu.VMEM((nz, quarter, DK), F32),
            pltpu.VMEM((nz, quarter, DK), F32),
            pltpu.VMEM((DV, DK), F32),
            pltpu.VMEM((2, DV, DK), F32),
            pltpu.VMEM((blocks, BT, NW), F32),
            pltpu.VMEM((ny - 1, mine, NW), F32),
            pltpu.VMEM((rows, DK), F32),
            pltpu.VMEM((mine, width), F32),
            pltpu.VMEM((width // (nx * nz * 2), NW), F32),
            pltpu.VMEM((ny - 1, width, NW), F32),
            dma((5,)),
            dma((2,)),
            dma((2,)),
            dma((2, nz - 1)),
            dma((2, nx - 1)),
            dma((2, nz - 1)),
            dma((2,)),
            dma((2, ny - 1, blocks // ny)),
            dma((2,)),
            dma((2, ny - 1)),
            dma((2, ny - 1, 2)),
            dma((2, ny - 1, 2)),
            dma((2, ny - 1, 2)),
            dma((2, ny - 1, 2)),
            dma((2, ny - 1, nx)),
        ],
        compiler_params=pltpu.CompilerParams(
            collective_id=0, has_side_effects=True, vmem_limit_bytes=62 * 2**20),
        cost_estimate=pl.CostEstimate(
            flops=40_000_000_000, bytes_accessed=30_000_000, transcendentals=1_000_000),
    )(tokens, w_query, w_key, w_value, w_gate, gate_rate.reshape(1, DK), out_grad)

    return mixed, signal


def solution(mesh, shape=(4, 4)):
    nx, nz = shape
    ny = mesh.shape["tp"]
    torus = Mesh(mesh.devices.reshape(nx, nz, 2, ny), SEQ_TP)
    placed = (
        P(SEQ, None),
        P(None, "tp"),
        P(None, "tp"),
        P(None, "tp"),
        P(None, "tp"),
        P("tp"),
        P(SEQ, "tp"),
    )
    return jax.shard_map(
        functools.partial(per_device, (nx, nz, ny)),
        mesh=torus,
        in_specs=placed,
        out_specs=(P(SEQ_TP, None), P(SEQ, "tp")),
        check_vma=False,
    )
```

```python
import functools
import math

import jax
import jax.numpy as jnp
from jax import lax
from jax.experimental import pallas as pl
from jax.experimental.pallas import tpu as pltpu
from jax.sharding import Mesh
from jax.sharding import PartitionSpec as P

DK = 128
DV = 256
BT = 256
NW = 3 * DK + DV
SEQ = ("seq_0", "seq_1", "seq_2")
SEQ_TP = ("seq_0", "seq_1", "seq_2", "tp")
MESH = pl.DeviceIdType.MESH
F32 = jnp.float32
BF16 = jnp.bfloat16


def mm(a, b):
    return lax.dot_general(a, b, (((1,), (0,)), ((), ())), preferred_element_type=F32)


def mm_nt(a, b):
    return lax.dot_general(a, b, (((1,), (1,)), ((), ())), preferred_element_type=F32)


def mm_tn(a, b):
    return lax.dot_general(a, b, (((0,), (0,)), ((), ())), preferred_element_type=F32)


def split(a):
    high = a.astype(BF16)
    return high, (a - high.astype(F32)).astype(BF16)


def steps(ny):
    return sorted(range(1, ny), key=lambda o: (-min(o, ny - o), o))


def body(dims, signal_scale, tok_hbm, wq, wk, wv, wg, rate_ref, og_hbm, out_hbm, gs_hbm,
         w_s, tok_s, og_s, qt, kt, vs, cs, sq, tri, carry, spre, gpre, dmsg, dpart, zsend, zrecv, zexc,
         xsend, xrecv, fsend, frecv, psend, states, gsb, acc, wsend, wl,
         low, osend, orecv, ssend, srecv, gsend,
         load_sem, tok_sem, d_sem, z_sem, x_sem, f_sem, p_sem, out_sem,
         wy_sem, w1_sem, f1_sem, w2_sem, f2_sem, wd_sem, og_sem, s_sem, gs_sem):
    nx, nz, ny, rows, width, blocks = dims
    x, z, c, y = (lax.axis_index(a) for a in SEQ_TP)
    sgn = 1 - 2 * c
    per_chunk = blocks // ny
    quarter = DV // nz
    pairs = blocks // 2
    mine = rows // ny
    near = steps(ny)
    order = [o - 1 for o in near]

    ring = nx
    share = width // (ring * ring * 2)
    first = x + c * (z - x)
    second = z + c * (x - z)

    def place(a, b):
        return {"seq_0": a + c * (b - a), "seq_1": b + c * (a - b)}

    def wrap(v):
        return lax.rem(v + ring, ring)

    def share_at(a, b, part, parts):
        size = share // parts
        start = ((c * ring + a) * ring + b) * share + part * size
        return pl.ds(pl.multiple_of(start, 8), size)

    def group_at(a, part, parts):
        size = ring * share // parts
        start = (c * ring + a) * ring * share + part * size
        return pl.ds(pl.multiple_of(start, 8), size)

    def remote(src, dst, sems, i, to):
        return pltpu.make_async_remote_copy(
            src, dst, sems.at[(0, *i)], sems.at[(1, *i)], device_id=to, device_id_type=MESH)

    def wy_copy(o):
        dst = wl.at[o - 1, share_at(first, second, 0, 1)]
        return remote(wsend, dst, wy_sem, (o - 1,), {"tp": lax.rem(y + o, ny)})

    turns = (0, 1) if ring > 2 else (0,)

    def w1_copy(s, turn):
        ref = wl.at[s, share_at(first, second, 0, 1)]
        return remote(ref, ref, w1_sem, (s, turn), place(first, wrap(second + 1 - 2 * turn)))

    def f1_copy(s, turn):
        ref = wl.at[s, share_at(first, wrap(second - 1 + 2 * turn), turn, 2)]
        return remote(ref, ref, f1_sem, (s, turn), place(first, wrap(second + 1 - 2 * turn)))

    def w2_copy(s, turn, half):
        ref = wl.at[s, group_at(first, half, 2)]
        return remote(ref, ref, w2_sem, (s, turn, half), place(wrap(first + 1 - 2 * turn), second))

    def f2_copy(s, turn):
        ref = wl.at[s, group_at(wrap(first - 1 + 2 * turn), turn, 2)]
        return remote(ref, ref, f2_sem, (s, turn), place(wrap(first + 1 - 2 * turn), second))

    def wd_copy(s, n):
        ref = wl.at[s, group_at(lax.rem(first + n, ring), 0, 1)]
        return remote(ref, ref, wd_sem, (s, n), {"seq_2": 1 - c})

    def start_all(copy, s):
        for turn in turns:
            copy(s, turn).start()

    def arrive_all(copy, s):
        for turn in turns:
            copy(s, turn).wait_recv()

    barrier = pltpu.get_barrier_semaphore()
    xrecv[...] = jnp.zeros_like(xrecv)
    peers = [{"seq_2": 1 - c}]
    peers += [{"seq_0": lax.rem(x + d, nx)} for d in range(1, nx)]
    peers += [{"seq_1": lax.rem(z + d, nz)} for d in range(1, nz)]
    peers += [{"tp": lax.rem(y + d, ny)} for d in range(1, ny)]
    for peer in peers:
        pl.semaphore_signal(barrier, inc=1, device_id=peer, device_id_type=MESH)

    weight_loads = [
        pltpu.make_async_copy(wq, w_s.at[:, pl.ds(0, DK)], load_sem.at[0]),
        pltpu.make_async_copy(wk, w_s.at[:, pl.ds(DK, DK)], load_sem.at[1]),
        pltpu.make_async_copy(wv, w_s.at[:, pl.ds(2 * DK, DV)], load_sem.at[2]),
        pltpu.make_async_copy(wg, w_s.at[:, pl.ds(2 * DK + DV, DK)], load_sem.at[3]),
    ]
    grad_load = pltpu.make_async_copy(og_hbm, og_s, load_sem.at[4])

    def tok_copy(i):
        slot = lax.rem(i, 2)
        start = pl.multiple_of(i * 2 * BT, 2 * BT)
        return pltpu.make_async_copy(tok_hbm.at[pl.ds(start, 2 * BT)], tok_s.at[slot], tok_sem.at[slot])

    def chunk(j):
        return pl.ds(pl.multiple_of(j * mine, mine), mine)

    def block_rows(b):
        return pl.ds(pl.multiple_of(b * BT, BT), BT)

    def og_copy(m, o):
        return remote(osend.at[m], orecv.at[m], og_sem, (m,), {"tp": lax.rem(y + o, ny)})

    def state_copy(m, o):
        return remote(ssend.at[m], srecv.at[m], s_sem, (m,), {"tp": lax.rem(y + o, ny)})

    def signal_copy(m, o, i):
        return remote(gsend.at[m, block_rows(i)], gsb.at[block_rows(y * per_chunk + i)], gs_sem, (m, i),
                      {"tp": lax.rem(y - o + ny, ny)})

    for load in weight_loads:
        load.start()
    tok_copy(0).start()
    grad_load.start()

    at = lax.broadcasted_iota(jnp.int32, (BT, BT), 0)
    before = lax.broadcasted_iota(jnp.int32, (BT, BT), 1)
    tri[0] = (at >= before).astype(F32).astype(BF16)
    tri[1] = (at <= before).astype(F32).astype(BF16)
    carry[...] = jnp.zeros_like(carry)
    spre[0] = jnp.zeros((DV, DK), F32)
    gpre[0] = jnp.zeros((DV, DK), F32)
    rate = rate_ref[...]
    with jax.named_scope("wload"):
        for load in weight_loads:
            load.wait()
    wsend[...] = w_s[share_at(first, second, 0, 1), :].astype(F32)
    with jax.named_scope("barrier"):
        pl.semaphore_wait(barrier, len(peers))
    for s in order:
        wy_copy(s + 1).start()

    def absorb(b, qk, val, gate, rate_here, cot_rows):
        rows_b = block_rows(b)
        squashed = jax.nn.sigmoid(gate)
        sq[rows_b, :] = squashed
        high, low = split(-rate_here * squashed)
        running = mm(tri[0], high) + mm(tri[0], low) + carry[0:1, :]
        carry[0:1, :] = running[BT - 1:BT, :]
        cs[rows_b, :] = running
        q_here = qk[:, 0:DK].astype(BF16).astype(F32)
        k_here = qk[:, DK:2 * DK].astype(BF16).astype(F32)
        q_run = (q_here * jnp.exp(running)).astype(BF16)
        k_run = (k_here * jnp.exp(-running)).astype(BF16)
        v_here = val.astype(BF16)
        qt[rows_b, :] = q_run
        kt[rows_b, :] = k_run
        vs[rows_b, :] = v_here
        spre[b + 1] = spre[b] + mm_tn(v_here, k_run)
        gpre[b + 1] = gpre[b] + mm_tn(cot_rows, q_run)

    def gradients(b, s_in, g_out, last, rate_here):
        rows_b = block_rows(b)
        q_run = qt[rows_b, :]
        k_run = kt[rows_b, :]
        v_here = vs[rows_b, :]
        o_grad = og_s[rows_b, :]
        running = cs[rows_b, :]
        squashed = sq[rows_b, :]
        upper = tri[1].astype(F32)
        lower = tri[0].astype(F32)
        scores_t = (mm_nt(k_run, q_run) * upper).astype(BF16)
        d_scores = (mm_nt(o_grad, v_here) * lower).astype(BF16)
        d_scores_t = (mm_nt(v_here, o_grad) * upper).astype(BF16)
        state = s_in + spre[b]
        after = s_in + spre[b + 1]
        cotangent = g_out + (gpre[last] - gpre[b + 1])
        state_low = state.astype(BF16)
        cot_low = cotangent.astype(BF16)
        dv = mm(scores_t, o_grad) + mm_nt(k_run, cot_low)
        dq = mm(o_grad, state_low) + mm(d_scores, k_run)
        dk = mm(v_here, cot_low) + mm(d_scores_t, q_run)
        boundary = jnp.sum(after * cotangent, axis=0, keepdims=True)
        high, low = split(q_run.astype(F32) * dq - k_run.astype(F32) * dk)
        dg = mm(tri[1], high) + mm(tri[1], low) + boundary
        pre = dg * (-rate_here) * squashed * (1.0 - squashed)
        return dq * jnp.exp(running), dk * jnp.exp(-running), dv, pre

    def put(ref, rows_b, parts):
        dq, dk, dv, pre = parts
        ref[rows_b, 0:DK] = dq.astype(ref.dtype)
        ref[rows_b, DK:2 * DK] = dk.astype(ref.dtype)
        ref[rows_b, 2 * DK:2 * DK + DV] = dv.astype(ref.dtype)
        ref[rows_b, 2 * DK + DV:] = pre.astype(ref.dtype)

    with jax.named_scope("proj"):
        @pl.loop(0, pairs)
        def _(i):
            @pl.when(i + 1 < pairs)
            def _():
                tok_copy(i + 1).start()

            @pl.when(i == 0)
            def _():
                grad_load.wait()

            @pl.when(i == pairs - 2)
            def _():
                for s in order[:2]:
                    wy_copy(s + 1).wait_recv()
                    start_all(w1_copy, s)

            @pl.when(i == pairs - 1)
            def _():
                for s in order[2:]:
                    wy_copy(s + 1).wait_recv()
                    start_all(w1_copy, s)
                for s in order[:1]:
                    arrive_all(w1_copy, s)
                    if ring > 2:
                        start_all(f1_copy, s)

            tok_copy(i).wait()
            here = tok_s[lax.rem(i, 2)]
            qk = mm(here, w_s[:, 0:2 * DK])
            val = mm(here, w_s[:, 2 * DK:2 * DK + DV])
            gate = mm(here, w_s[:, 2 * DK + DV:])
            for half in range(2):
                b = i * 2 + half
                part = slice(half * BT, (half + 1) * BT)
                absorb(b, qk[part], val[part], gate[part], rate, og_s[block_rows(b), :])

    x_chunk = pltpu.make_async_copy(tok_hbm.at[chunk(y)], tok_s.at[0, pl.ds(0, mine)], tok_sem.at[0])
    x_chunk.start()
    for s in order[1:]:
        arrive_all(w1_copy, s)
        if ring > 2:
            start_all(f1_copy, s)

    def start_w2(s, halves=(0, 1)):
        if ring > 2 and 0 in halves:
            arrive_all(f1_copy, s)
        for half in halves:
            for turn in turns:
                w2_copy(s, turn, half).start()

    def arrive_w2(s):
        for half in range(2):
            for turn in turns:
                w2_copy(s, turn, half).wait_recv()

    @pl.when(c == 0)
    def _():
        start_w2(order[0])
    log_total = carry[0:1, :]
    decay = jnp.exp(log_total)
    dmsg[0, 0:DV, :] = spre[blocks] * decay
    dmsg[1, 0:DV, :] = gpre[blocks]
    for kind in range(2):
        dmsg[kind, DV:DV + 8, :] = jnp.broadcast_to(log_total, (8, DK))

    d_copy = pltpu.make_async_remote_copy(
        dmsg.at[1 - c], dpart, d_sem.at[0], d_sem.at[1], device_id={"seq_2": 1 - c}, device_id_type=MESH)
    with jax.named_scope("d2d"):
        d_copy.start()
        d_copy.wait()

    chip_log = log_total + dpart[DV:DV + 1, :]
    chip = dpart[0:DV, :] + jnp.exp(dpart[DV:DV + 1, :]) * dmsg[c, 0:DV, :]
    for n in range(nz):
        zsend[n, 0:quarter, :] = chip[n * quarter:(n + 1) * quarter, :]
        zsend[n, quarter:quarter + 8, :] = jnp.broadcast_to(chip_log, (8, DK))
    zrecv[z] = zsend[z]
    z_copies = []
    for d in range(1, nz):
        to = lax.rem(z + d, nz)
        z_copies.append(pltpu.make_async_remote_copy(
            zsend.at[to], zrecv.at[z], z_sem.at[0, d - 1], z_sem.at[1, d - 1],
            device_id={"seq_1": to}, device_id_type=MESH))
    for copy in z_copies:
        copy.start()
    for m, o in enumerate(near):
        osend[m] = og_s[chunk(lax.rem(y + o, ny)), :].astype(F32)
    for m, o in enumerate(near):
        og_copy(m, o).start()
    @pl.when(c == 1)
    def _():
        start_w2(order[0])

    with jax.named_scope("zex"):
        for copy in z_copies:
            copy.wait()

    total = jnp.zeros((quarter, DK), F32)
    total_log = jnp.zeros((1, DK), F32)
    for n in range(nz):
        src = c * (nz - 1) + sgn * n
        zexc[src, 0:quarter, :] = total
        zexc[src, quarter:quarter + 8, :] = jnp.broadcast_to(total_log, (8, DK))
        log_here = zrecv[src, quarter:quarter + 1, :]
        total = zrecv[src, 0:quarter, :] + jnp.exp(log_here) * total
        total_log = total_log + log_here
    xsend[0:quarter, :] = total
    xsend[quarter:quarter + 8, :] = jnp.broadcast_to(total_log, (8, DK))

    def x_copy(d):
        to = x + sgn * d
        inside = (to >= 0) & (to < nx)
        return inside, pltpu.make_async_remote_copy(
            xsend, xrecv.at[d - 1], x_sem.at[0, d - 1], x_sem.at[1, d - 1],
            device_id={"seq_0": jnp.where(inside, to, 1 - jnp.minimum(x, 1))}, device_id_type=MESH)

    for d in range(1, nx):
        inside, copy = x_copy(d)
        pl.when(inside)(copy.start)

    for s in order[1:2]:
        start_w2(s, (0,))

    @pl.when(c == 0)
    def _():
        for s in order[1:2]:
            start_w2(s, (1,))

    with jax.named_scope("xex"):
        for d in range(1, nx):
            inside, copy = x_copy(d)
            pl.when(inside)(copy.wait_send)
            source = x - sgn * d
            pl.when((source >= 0) & (source < nx))(copy.wait_recv)

    entering = jnp.zeros((quarter, DK), F32)
    for d in reversed(range(1, nx)):
        entering = xrecv[d - 1, 0:quarter, :] + jnp.exp(xrecv[d - 1, quarter:quarter + 1, :]) * entering
    for n in range(nz):
        fsend[n] = zexc[n, 0:quarter, :] + jnp.exp(zexc[n, quarter:quarter + 1, :]) * entering
    frecv[z] = fsend[z]
    f_copies = []
    for d in range(1, nz):
        to = lax.rem(z + d, nz)
        f_copies.append(pltpu.make_async_remote_copy(
            fsend.at[to], frecv.at[z], f_sem.at[0, d - 1], f_sem.at[1, d - 1],
            device_id={"seq_1": to}, device_id_type=MESH))
    for copy in f_copies:
        copy.start()

    @pl.when(c == 1)
    def _():
        for s in order[1:2]:
            start_w2(s, (1,))

    with jax.named_scope("fex"):
        for copy in f_copies:
            copy.wait()

    entered = frecv[...].reshape(DV, DK)
    psend[...] = dmsg[c, 0:DV, :] + decay * entered
    states[c] = entered
    p_copy = pltpu.make_async_remote_copy(
        psend, states.at[c], p_sem.at[0], p_sem.at[1], device_id={"seq_2": 1 - c}, device_id_type=MESH)
    def group_done(s):
        if ring > 2:
            start_all(f2_copy, s)
        for n in sorted({0, 1, ring - 1}):
            wd_copy(s, n).start()

    def whole(s):
        if ring > 2:
            arrive_all(f2_copy, s)
            wd_copy(s, 2).start()
        for n in range(ring):
            wd_copy(s, n).wait_recv()

    p_copy.start()
    with jax.named_scope("w2z"):
        arrive_w2(order[0])
        group_done(order[0])
    with jax.named_scope("pex"):
        p_copy.wait()

    states[1] = states[1] * decay
    for m, o in enumerate(near):
        to = lax.rem(y + o, ny)
        start_log = cs[pl.ds(pl.multiple_of(jnp.maximum(to * mine - 8, 0), 8), 8), :][7:8, :]
        start_log = jnp.where(to > 0, start_log, 0.0)
        ssend[m, 0, 0:DV, :] = (states[0] + spre[to * per_chunk]) * jnp.exp(start_log)
        ssend[m, 1, 0:DV, :] = (states[1] + (gpre[blocks] - gpre[(to + 1) * per_chunk])) * jnp.exp(-start_log)
        ssend[m, 0, DV:DV + 8, :] = jnp.broadcast_to(rate, (8, DK))
        ssend[m, 1, DV:DV + 8, :] = jnp.broadcast_to(rate, (8, DK))

    for m, o in enumerate(near):
        state_copy(m, o).start()

    with jax.named_scope("own"):
        for i in range(per_chunk):
            b = y * per_chunk + i
            parts = gradients(b, states[0], states[1], blocks, rate)
            gsb[block_rows(b), :] = parts[3] * signal_scale
            put(low, block_rows(i), parts)
    with jax.named_scope("w2a"):
        for s in order[1:2]:
            arrive_w2(s)
            group_done(s)
        for s in order[2:]:
            start_w2(s)
    cols = min(512, width)

    def mix(grads, weights, last):
        @pl.loop(0, width // cols)
        def _(i):
            at = pl.ds(pl.multiple_of(i * cols, cols), cols)
            term = mm_nt(grads, weights(at))
            if last is None:
                acc[:, at] = term
            elif last:
                tok_s[1, 0:mine, at] = (acc[:, at] + term).astype(BF16)
            else:
                acc[:, at] = acc[:, at] + term

    def fill(s, m):
        carry[...] = jnp.zeros_like(carry)
        spre[0] = jnp.zeros((DV, DK), F32)
        gpre[0] = jnp.zeros((DV, DK), F32)
        here = tok_s[0, 0:mine, :]
        qk = mm(here, wl[s, :, 0:2 * DK].astype(BF16))
        val = mm(here, wl[s, :, 2 * DK:2 * DK + DV].astype(BF16))
        gate = mm(here, wl[s, :, 2 * DK + DV:].astype(BF16))
        if m == min(1, len(near) - 1):
            with jax.named_scope("w2c"):
                for later in order[2:]:
                    arrive_w2(later)
                    group_done(later)
        with jax.named_scope(f"ogw{m}"):
            og_copy(m, near[m]).wait_recv()
        with jax.named_scope(f"stw{m}"):
            state_copy(m, near[m]).wait_recv()
        og_s[0:mine, :] = orecv[m].astype(BF16)
        rate_here = srecv[m, 0, DV:DV + 1, :]
        for i in range(per_chunk):
            part = slice(i * BT, (i + 1) * BT)
            absorb(i, qk[part], val[part], gate[part], rate_here, og_s[block_rows(i), :])
        for i in range(per_chunk):
            parts = gradients(i, srecv[m, 0, 0:DV, :], srecv[m, 1, 0:DV, :], per_chunk, rate_here)
            gsend[m, block_rows(i), :] = parts[3] * signal_scale
            put(low, block_rows(i), parts)
            signal_copy(m, near[m], i).start()

    with jax.named_scope("mix_own"):
        mix(low[...], lambda at: w_s[at, :], None)
    x_chunk.wait()
    for m, o in enumerate(near):
        s = o - 1
        with jax.named_scope(f"whole{m}"):
            whole(s)
        with jax.named_scope(f"fill{m}"):
            fill(s, m)
        with jax.named_scope(f"mix{m}"):
            mix(low[...], lambda at: wl[s, at, :].astype(BF16), s == order[-1])
    out_copy = pltpu.make_async_copy(tok_s.at[1, pl.ds(0, mine)], out_hbm, out_sem.at[1])
    out_copy.start()
    with jax.named_scope("end"):
        for m, o in enumerate(near):
            for i in range(per_chunk):
                signal_copy(m, o, i).wait_recv()
        gs_copy = pltpu.make_async_copy(gsb, gs_hbm, out_sem.at[0])
        gs_copy.start()
        for s in order:
            wy_copy(s + 1).wait_send()
            for turn in turns:
                w1_copy(s, turn).wait_send()
                w2_copy(s, turn, 0).wait_send()
                w2_copy(s, turn, 1).wait_send()
                if ring > 2:
                    f1_copy(s, turn).wait_send()
                    f2_copy(s, turn).wait_send()
            for n in range(ring):
                wd_copy(s, n).wait_send()
        for m, o in enumerate(near):
            og_copy(m, o).wait_send()
            state_copy(m, o).wait_send()
            for i in range(per_chunk):
                signal_copy(m, o, i).wait_send()
        out_copy.wait()
        gs_copy.wait()


def per_device(dims, tokens, w_query, w_key, w_value, w_gate, gate_rate, out_grad):
    nx, nz, ny = dims
    rows, width = tokens.shape
    blocks = rows // BT
    mine = rows // ny
    quarter = DV // nz
    whole_tokens = rows * nx * nz * 2
    signal_scale = 4.0 * math.sqrt(whole_tokens * DK / DV)

    count_near = ny - 1
    any_spec = pl.BlockSpec(memory_space=pl.ANY)
    vmem_spec = pl.BlockSpec(memory_space=pltpu.VMEM)
    dma = pltpu.SemaphoreType.DMA
    mixed, signal = pl.pallas_call(
        functools.partial(body, (nx, nz, ny, rows, width, blocks), signal_scale),
        out_shape=(
            jax.ShapeDtypeStruct((mine, width), BF16),
            jax.ShapeDtypeStruct((rows, DK), F32),
        ),
        in_specs=[any_spec] * 5 + [vmem_spec, any_spec],
        out_specs=(any_spec, any_spec),
        scratch_shapes=[
            pltpu.VMEM((width, NW), BF16),
            pltpu.VMEM((2, 2 * BT, width), BF16),
            pltpu.VMEM((rows, DV), BF16),
            pltpu.VMEM((rows, DK), BF16),
            pltpu.VMEM((rows, DK), BF16),
            pltpu.VMEM((rows, DV), BF16),
            pltpu.VMEM((rows, DK), F32),
            pltpu.VMEM((rows, DK), F32),
            pltpu.VMEM((2, BT, BT), BF16),
            pltpu.VMEM((8, DK), F32),
            pltpu.VMEM((blocks + 1, DV, DK), F32),
            pltpu.VMEM((blocks + 1, DV, DK), F32),
            pltpu.VMEM((2, DV + 8, DK), F32),
            pltpu.VMEM((DV + 8, DK), F32),
            pltpu.VMEM((nz, quarter + 8, DK), F32),
            pltpu.VMEM((nz, quarter + 8, DK), F32),
            pltpu.VMEM((nz, quarter + 8, DK), F32),
            pltpu.VMEM((quarter + 8, DK), F32),
            pltpu.VMEM((nx - 1, quarter + 8, DK), F32),
            pltpu.VMEM((nz, quarter, DK), F32),
            pltpu.VMEM((nz, quarter, DK), F32),
            pltpu.VMEM((DV, DK), F32),
            pltpu.VMEM((2, DV, DK), F32),
            pltpu.VMEM((rows, DK), F32),
            pltpu.VMEM((mine, width), F32),
            pltpu.VMEM((width // (nx * nz * 2), NW), F32),
            pltpu.VMEM((ny - 1, width, NW), F32),
            pltpu.VMEM((mine, NW), BF16),
            pltpu.VMEM((count_near, mine, DV), F32),
            pltpu.VMEM((count_near, mine, DV), F32),
            pltpu.VMEM((count_near, 2, DV + 8, DK), F32),
            pltpu.VMEM((count_near, 2, DV + 8, DK), F32),
            pltpu.VMEM((count_near, mine, DK), F32),
            dma((5,)),
            dma((2,)),
            dma((2,)),
            dma((2, nz - 1)),
            dma((2, nx - 1)),
            dma((2, nz - 1)),
            dma((2,)),
            dma((2,)),
            dma((2, ny - 1)),
            dma((2, ny - 1, 2)),
            dma((2, ny - 1, 2)),
            dma((2, ny - 1, 2, 2)),
            dma((2, ny - 1, 2)),
            dma((2, ny - 1, nx)),
            dma((2, count_near)),
            dma((2, count_near)),
            dma((2, count_near, blocks // ny)),
        ],
        compiler_params=pltpu.CompilerParams(
            collective_id=0, has_side_effects=True, vmem_limit_bytes=62 * 2**20),
        cost_estimate=pl.CostEstimate(
            flops=40_000_000_000, bytes_accessed=30_000_000, transcendentals=1_000_000),
    )(tokens, w_query, w_key, w_value, w_gate, gate_rate.reshape(1, DK), out_grad)

    return mixed, signal


def solution(mesh, shape=(4, 4)):
    nx, nz = shape
    ny = mesh.shape["tp"]
    torus = Mesh(mesh.devices.reshape(nx, nz, 2, ny), SEQ_TP)
    placed = (
        P(SEQ, None),
        P(None, "tp"),
        P(None, "tp"),
        P(None, "tp"),
        P(None, "tp"),
        P("tp"),
        P(SEQ, "tp"),
    )
    return jax.shard_map(
        functools.partial(per_device, (nx, nz, ny)),
        mesh=torus,
        in_specs=placed,
        out_specs=(P(SEQ_TP, None), P(SEQ, "tp")),
        check_vma=False,
    )
```

```python
import functools
import math

import jax
import jax.numpy as jnp
from jax import lax
from jax.experimental import pallas as pl
from jax.experimental.pallas import tpu as pltpu
from jax.sharding import Mesh
from jax.sharding import PartitionSpec as P

DK = 128
DV = 256
BT = 256
NW = 3 * DK + DV
SEQ = ("seq_0", "seq_1", "seq_2")
SEQ_TP = ("seq_0", "seq_1", "seq_2", "tp")
MESH = pl.DeviceIdType.MESH
F32 = jnp.float32
BF16 = jnp.bfloat16


def mm(a, b):
    return lax.dot_general(a, b, (((1,), (0,)), ((), ())), preferred_element_type=F32)


def mm_nt(a, b):
    return lax.dot_general(a, b, (((1,), (1,)), ((), ())), preferred_element_type=F32)


def mm_tn(a, b):
    return lax.dot_general(a, b, (((0,), (0,)), ((), ())), preferred_element_type=F32)


def split(a):
    high = a.astype(BF16)
    return high, (a - high.astype(F32)).astype(BF16)


def steps(ny):
    return sorted(range(1, ny), key=lambda o: (-min(o, ny - o), o))


def body(dims, signal_scale, tok_hbm, wq, wk, wv, wg, rate_ref, og_hbm, out_hbm, gs_hbm,
         w_s, tok_s, og_s, qt, kt, vs, cs, sq, tri, carry, spre, gpre, dmsg, dpart, zsend, zrecv, zexc,
         xsend, xrecv, fsend, frecv, psend, states, gsb, acc, wsend, wl,
         low, osend, orecv, ssend, srecv, gsend,
         load_sem, tok_sem, d_sem, z_sem, x_sem, f_sem, p_sem, out_sem,
         wy_sem, w1_sem, f1_sem, w2_sem, f2_sem, wd_sem, og_sem, s_sem, gs_sem):
    nx, nz, ny, rows, width, blocks = dims
    x, z, c, y = (lax.axis_index(a) for a in SEQ_TP)
    sgn = 1 - 2 * c
    per_chunk = blocks // ny
    quarter = DV // nz
    pairs = blocks // 2
    mine = rows // ny
    near = steps(ny)
    order = [o - 1 for o in near]

    ring = nx
    share = width // (ring * ring * 2)
    first = x + c * (z - x)
    second = z + c * (x - z)

    def place(a, b):
        return {"seq_0": a + c * (b - a), "seq_1": b + c * (a - b)}

    def wrap(v):
        return lax.rem(v + ring, ring)

    def share_at(a, b, part, parts):
        size = share // parts
        start = ((c * ring + a) * ring + b) * share + part * size
        return pl.ds(pl.multiple_of(start, 8), size)

    def group_at(a, part, parts):
        size = ring * share // parts
        start = (c * ring + a) * ring * share + part * size
        return pl.ds(pl.multiple_of(start, 8), size)

    def remote(src, dst, sems, i, to):
        return pltpu.make_async_remote_copy(
            src, dst, sems.at[(0, *i)], sems.at[(1, *i)], device_id=to, device_id_type=MESH)

    def wy_copy(o):
        dst = wl.at[o - 1, share_at(first, second, 0, 1)]
        return remote(wsend, dst, wy_sem, (o - 1,), {"tp": lax.rem(y + o, ny)})

    turns = (0, 1) if ring > 2 else (0,)

    def w1_copy(s, turn):
        ref = wl.at[s, share_at(first, second, 0, 1)]
        return remote(ref, ref, w1_sem, (s, turn), place(first, wrap(second + 1 - 2 * turn)))

    def f1_copy(s, turn):
        ref = wl.at[s, share_at(first, wrap(second - 1 + 2 * turn), turn, 2)]
        return remote(ref, ref, f1_sem, (s, turn), place(first, wrap(second + 1 - 2 * turn)))

    def w2_copy(s, turn, half):
        ref = wl.at[s, group_at(first, half, 2)]
        return remote(ref, ref, w2_sem, (s, turn, half), place(wrap(first + 1 - 2 * turn), second))

    def f2_copy(s, turn):
        ref = wl.at[s, group_at(wrap(first - 1 + 2 * turn), turn, 2)]
        return remote(ref, ref, f2_sem, (s, turn), place(wrap(first + 1 - 2 * turn), second))

    def wd_copy(s, n):
        ref = wl.at[s, group_at(lax.rem(first + n, ring), 0, 1)]
        return remote(ref, ref, wd_sem, (s, n), {"seq_2": 1 - c})

    def start_all(copy, s):
        for turn in turns:
            copy(s, turn).start()

    def arrive_all(copy, s):
        for turn in turns:
            copy(s, turn).wait_recv()

    barrier = pltpu.get_barrier_semaphore()
    xrecv[...] = jnp.zeros_like(xrecv)
    peers = [{"seq_2": 1 - c}]
    peers += [{"seq_0": lax.rem(x + d, nx)} for d in range(1, nx)]
    peers += [{"seq_1": lax.rem(z + d, nz)} for d in range(1, nz)]
    peers += [{"tp": lax.rem(y + d, ny)} for d in range(1, ny)]
    for peer in peers:
        pl.semaphore_signal(barrier, inc=1, device_id=peer, device_id_type=MESH)

    weight_loads = [
        pltpu.make_async_copy(wq, w_s.at[:, pl.ds(0, DK)], load_sem.at[0]),
        pltpu.make_async_copy(wk, w_s.at[:, pl.ds(DK, DK)], load_sem.at[1]),
        pltpu.make_async_copy(wv, w_s.at[:, pl.ds(2 * DK, DV)], load_sem.at[2]),
        pltpu.make_async_copy(wg, w_s.at[:, pl.ds(2 * DK + DV, DK)], load_sem.at[3]),
    ]
    grad_load = pltpu.make_async_copy(og_hbm, og_s, load_sem.at[4])

    def tok_copy(i):
        slot = lax.rem(i, 2)
        start = pl.multiple_of(i * 2 * BT, 2 * BT)
        return pltpu.make_async_copy(tok_hbm.at[pl.ds(start, 2 * BT)], tok_s.at[slot], tok_sem.at[slot])

    def chunk(j):
        return pl.ds(pl.multiple_of(j * mine, mine), mine)

    def block_rows(b):
        return pl.ds(pl.multiple_of(b * BT, BT), BT)

    def og_copy(m, o):
        return remote(osend.at[m], orecv.at[m], og_sem, (m,), {"tp": lax.rem(y + o, ny)})

    def state_copy(m, o):
        return remote(ssend.at[m], srecv.at[m], s_sem, (m,), {"tp": lax.rem(y + o, ny)})

    def signal_copy(m, o, i):
        return remote(gsend.at[m, block_rows(i)], gsb.at[block_rows(y * per_chunk + i)], gs_sem, (m, i),
                      {"tp": lax.rem(y - o + ny, ny)})

    for load in weight_loads:
        load.start()
    tok_copy(0).start()
    grad_load.start()

    at = lax.broadcasted_iota(jnp.int32, (BT, BT), 0)
    before = lax.broadcasted_iota(jnp.int32, (BT, BT), 1)
    tri[0] = (at >= before).astype(F32).astype(BF16)
    tri[1] = (at <= before).astype(F32).astype(BF16)
    carry[...] = jnp.zeros_like(carry)
    spre[0] = jnp.zeros((DV, DK), F32)
    gpre[0] = jnp.zeros((DV, DK), F32)
    rate = rate_ref[...]
    with jax.named_scope("wload"):
        for load in weight_loads:
            load.wait()
    wsend[...] = w_s[share_at(first, second, 0, 1), :].astype(F32)
    with jax.named_scope("barrier"):
        pl.semaphore_wait(barrier, len(peers))
    for s in order:
        wy_copy(s + 1).start()

    def absorb(first_b, qk, val, gate, rate_here):
        count = qk.shape[0] // BT
        parts = [slice(n * BT, (n + 1) * BT) for n in range(count)]
        squashed = [jax.nn.sigmoid(gate[part]) for part in parts]
        pieces = [split(-rate_here * part) for part in squashed]
        running = [mm(tri[0], high) + mm(tri[0], low) for high, low in pieces]
        base = carry[0:1, :]
        for n in range(count):
            running[n] = running[n] + base
            base = running[n][BT - 1:BT, :]
        carry[0:1, :] = base
        q_run = [(qk[parts[n], 0:DK].astype(BF16).astype(F32) * jnp.exp(running[n])).astype(BF16) for n in range(count)]
        k_run = [(qk[parts[n], DK:2 * DK].astype(BF16).astype(F32) * jnp.exp(-running[n])).astype(BF16)
                 for n in range(count)]
        v_here = [val[part].astype(BF16) for part in parts]
        s_terms = [mm_tn(v_here[n], k_run[n]) for n in range(count)]
        g_terms = [mm_tn(og_s[block_rows(first_b + n), :], q_run[n]) for n in range(count)]
        s_sum, g_sum = spre[first_b], gpre[first_b]
        for n in range(count):
            rows_b = block_rows(first_b + n)
            s_sum = s_sum + s_terms[n]
            g_sum = g_sum + g_terms[n]
            sq[rows_b, :] = squashed[n]
            cs[rows_b, :] = running[n]
            qt[rows_b, :] = q_run[n]
            kt[rows_b, :] = k_run[n]
            vs[rows_b, :] = v_here[n]
            spre[first_b + n + 1] = s_sum
            gpre[first_b + n + 1] = g_sum

    def gradients(b, s_in, g_out, last, rate_here):
        rows_b = block_rows(b)
        q_run = qt[rows_b, :]
        k_run = kt[rows_b, :]
        v_here = vs[rows_b, :]
        o_grad = og_s[rows_b, :]
        running = cs[rows_b, :]
        squashed = sq[rows_b, :]
        upper = tri[1].astype(F32)
        lower = tri[0].astype(F32)
        scores_t = (mm_nt(k_run, q_run) * upper).astype(BF16)
        d_scores = (mm_nt(o_grad, v_here) * lower).astype(BF16)
        d_scores_t = (mm_nt(v_here, o_grad) * upper).astype(BF16)
        state = s_in + spre[b]
        after = s_in + spre[b + 1]
        cotangent = g_out + (gpre[last] - gpre[b + 1])
        state_low = state.astype(BF16)
        cot_low = cotangent.astype(BF16)
        dv = mm(scores_t, o_grad) + mm_nt(k_run, cot_low)
        dq = mm(o_grad, state_low) + mm(d_scores, k_run)
        dk = mm(v_here, cot_low) + mm(d_scores_t, q_run)
        boundary = jnp.sum(after * cotangent, axis=0, keepdims=True)
        high, low = split(q_run.astype(F32) * dq - k_run.astype(F32) * dk)
        dg = mm(tri[1], high) + mm(tri[1], low) + boundary
        pre = dg * (-rate_here) * squashed * (1.0 - squashed)
        return dq * jnp.exp(running), dk * jnp.exp(-running), dv, pre

    def put(ref, rows_b, parts):
        dq, dk, dv, pre = parts
        ref[rows_b, 0:DK] = dq.astype(ref.dtype)
        ref[rows_b, DK:2 * DK] = dk.astype(ref.dtype)
        ref[rows_b, 2 * DK:2 * DK + DV] = dv.astype(ref.dtype)
        ref[rows_b, 2 * DK + DV:] = pre.astype(ref.dtype)

    with jax.named_scope("proj"):
        @pl.loop(0, pairs)
        def _(i):
            @pl.when(i + 1 < pairs)
            def _():
                tok_copy(i + 1).start()

            @pl.when(i == 0)
            def _():
                grad_load.wait()

            @pl.when(i == pairs - 2)
            def _():
                for s in order[:2]:
                    wy_copy(s + 1).wait_recv()
                    start_all(w1_copy, s)

            @pl.when(i == pairs - 1)
            def _():
                for s in order[2:]:
                    wy_copy(s + 1).wait_recv()
                    start_all(w1_copy, s)
                for s in order[:1]:
                    arrive_all(w1_copy, s)
                    if ring > 2:
                        start_all(f1_copy, s)

            tok_copy(i).wait()
            here = tok_s[lax.rem(i, 2)]
            qk = mm(here, w_s[:, 0:2 * DK])
            val = mm(here, w_s[:, 2 * DK:2 * DK + DV])
            gate = mm(here, w_s[:, 2 * DK + DV:])
            absorb(i * 2, qk, val, gate, rate)

    x_chunk = pltpu.make_async_copy(tok_hbm.at[chunk(y)], tok_s.at[0, pl.ds(0, mine)], tok_sem.at[0])
    x_chunk.start()
    for s in order[1:]:
        arrive_all(w1_copy, s)
        if ring > 2:
            start_all(f1_copy, s)

    def start_w2(s, halves=(0, 1)):
        if ring > 2 and 0 in halves:
            arrive_all(f1_copy, s)
        for half in halves:
            for turn in turns:
                w2_copy(s, turn, half).start()

    def arrive_w2(s):
        for half in range(2):
            for turn in turns:
                w2_copy(s, turn, half).wait_recv()

    log_total = carry[0:1, :]
    decay = jnp.exp(log_total)
    dmsg[0, 0:DV, :] = spre[blocks] * decay
    dmsg[1, 0:DV, :] = gpre[blocks]
    for kind in range(2):
        dmsg[kind, DV:DV + 8, :] = jnp.broadcast_to(log_total, (8, DK))

    d_copy = pltpu.make_async_remote_copy(
        dmsg.at[1 - c], dpart, d_sem.at[0], d_sem.at[1], device_id={"seq_2": 1 - c}, device_id_type=MESH)
    with jax.named_scope("d2d"):
        d_copy.start()
        start_w2(order[0], (0,))
        d_copy.wait()

    chip_log = log_total + dpart[DV:DV + 1, :]
    chip = dpart[0:DV, :] + jnp.exp(dpart[DV:DV + 1, :]) * dmsg[c, 0:DV, :]
    for n in range(nz):
        zsend[n, 0:quarter, :] = chip[n * quarter:(n + 1) * quarter, :]
        zsend[n, quarter:quarter + 8, :] = jnp.broadcast_to(chip_log, (8, DK))
    zrecv[z] = zsend[z]
    z_copies = []
    for d in range(1, nz):
        to = lax.rem(z + d, nz)
        z_copies.append(pltpu.make_async_remote_copy(
            zsend.at[to], zrecv.at[z], z_sem.at[0, d - 1], z_sem.at[1, d - 1],
            device_id={"seq_1": to}, device_id_type=MESH))
    for copy in z_copies:
        copy.start()
    for m, o in enumerate(near):
        osend[m] = og_s[chunk(lax.rem(y + o, ny)), :].astype(F32)
    for m, o in enumerate(near):
        og_copy(m, o).start()
    start_w2(order[0], (1,))

    with jax.named_scope("zex"):
        for copy in z_copies:
            copy.wait()

    total = jnp.zeros((quarter, DK), F32)
    total_log = jnp.zeros((1, DK), F32)
    for n in range(nz):
        src = c * (nz - 1) + sgn * n
        zexc[src, 0:quarter, :] = total
        zexc[src, quarter:quarter + 8, :] = jnp.broadcast_to(total_log, (8, DK))
        log_here = zrecv[src, quarter:quarter + 1, :]
        total = zrecv[src, 0:quarter, :] + jnp.exp(log_here) * total
        total_log = total_log + log_here
    xsend[0:quarter, :] = total
    xsend[quarter:quarter + 8, :] = jnp.broadcast_to(total_log, (8, DK))

    def x_copy(d):
        to = x + sgn * d
        inside = (to >= 0) & (to < nx)
        return inside, pltpu.make_async_remote_copy(
            xsend, xrecv.at[d - 1], x_sem.at[0, d - 1], x_sem.at[1, d - 1],
            device_id={"seq_0": jnp.where(inside, to, 1 - jnp.minimum(x, 1))}, device_id_type=MESH)

    for d in range(1, nx):
        inside, copy = x_copy(d)
        pl.when(inside)(copy.start)

    for s in order[1:2]:
        start_w2(s, (0,))

    @pl.when(c == 0)
    def _():
        for s in order[1:2]:
            start_w2(s, (1,))

    with jax.named_scope("xex"):
        for d in range(1, nx):
            inside, copy = x_copy(d)
            pl.when(inside)(copy.wait_send)
            source = x - sgn * d
            pl.when((source >= 0) & (source < nx))(copy.wait_recv)

    entering = jnp.zeros((quarter, DK), F32)
    for d in reversed(range(1, nx)):
        entering = xrecv[d - 1, 0:quarter, :] + jnp.exp(xrecv[d - 1, quarter:quarter + 1, :]) * entering
    for n in range(nz):
        fsend[n] = zexc[n, 0:quarter, :] + jnp.exp(zexc[n, quarter:quarter + 1, :]) * entering
    frecv[z] = fsend[z]
    f_copies = []
    for d in range(1, nz):
        to = lax.rem(z + d, nz)
        f_copies.append(pltpu.make_async_remote_copy(
            fsend.at[to], frecv.at[z], f_sem.at[0, d - 1], f_sem.at[1, d - 1],
            device_id={"seq_1": to}, device_id_type=MESH))
    for copy in f_copies:
        copy.start()

    @pl.when(c == 1)
    def _():
        for s in order[1:2]:
            start_w2(s, (1,))

    with jax.named_scope("fex"):
        for copy in f_copies:
            copy.wait()

    entered = frecv[...].reshape(DV, DK)
    psend[...] = dmsg[c, 0:DV, :] + decay * entered
    states[c] = entered
    p_copy = pltpu.make_async_remote_copy(
        psend, states.at[c], p_sem.at[0], p_sem.at[1], device_id={"seq_2": 1 - c}, device_id_type=MESH)
    def group_done(s):
        if ring > 2:
            start_all(f2_copy, s)
        for n in sorted({0, 1, ring - 1}):
            wd_copy(s, n).start()

    def last_group(s):
        if ring > 2:
            arrive_all(f2_copy, s)
            wd_copy(s, 2).start()

    def whole(s):
        for n in range(ring):
            wd_copy(s, n).wait_recv()

    p_copy.start()
    with jax.named_scope("w2z"):
        arrive_w2(order[0])
        group_done(order[0])
    with jax.named_scope("pex"):
        p_copy.wait()

    states[1] = states[1] * decay
    for m, o in enumerate(near):
        to = lax.rem(y + o, ny)
        start_log = cs[pl.ds(pl.multiple_of(jnp.maximum(to * mine - 8, 0), 8), 8), :][7:8, :]
        start_log = jnp.where(to > 0, start_log, 0.0)
        ssend[m, 0, 0:DV, :] = (states[0] + spre[to * per_chunk]) * jnp.exp(start_log)
        ssend[m, 1, 0:DV, :] = (states[1] + (gpre[blocks] - gpre[(to + 1) * per_chunk])) * jnp.exp(-start_log)
        ssend[m, 0, DV:DV + 8, :] = jnp.broadcast_to(rate, (8, DK))
        ssend[m, 1, DV:DV + 8, :] = jnp.broadcast_to(rate, (8, DK))

    for m, o in enumerate(near):
        state_copy(m, o).start()

    with jax.named_scope("own"):
        made = [gradients(y * per_chunk + i, states[0], states[1], blocks, rate) for i in range(per_chunk)]
        for i in range(per_chunk):
            gsb[block_rows(y * per_chunk + i), :] = made[i][3] * signal_scale
            put(low, block_rows(i), made[i])
    with jax.named_scope("w2a"):
        for s in order[1:2]:
            arrive_w2(s)
            group_done(s)
        for s in order[2:]:
            start_w2(s)
    cols = width // 2

    def mix(grads, weights, last):
        @pl.loop(0, width // cols)
        def _(i):
            at = pl.ds(pl.multiple_of(i * cols, cols), cols)
            term = mm_nt(grads, weights(at))
            if last is None:
                acc[:, at] = term
            elif last:
                tok_s[1, 0:mine, at] = (acc[:, at] + term).astype(BF16)
            else:
                acc[:, at] = acc[:, at] + term

    def fill(s, m):
        carry[...] = jnp.zeros_like(carry)
        spre[0] = jnp.zeros((DV, DK), F32)
        gpre[0] = jnp.zeros((DV, DK), F32)
        here = tok_s[0, 0:mine, :]
        qk = mm(here, wl[s, :, 0:2 * DK].astype(BF16))
        val = mm(here, wl[s, :, 2 * DK:2 * DK + DV].astype(BF16))
        gate = mm(here, wl[s, :, 2 * DK + DV:].astype(BF16))
        if m == min(1, len(near) - 1):
            with jax.named_scope("w2c"):
                for later in order[2:]:
                    arrive_w2(later)
                    group_done(later)
        with jax.named_scope(f"ogw{m}"):
            og_copy(m, near[m]).wait_recv()
        with jax.named_scope(f"stw{m}"):
            state_copy(m, near[m]).wait_recv()
        og_s[0:mine, :] = orecv[m].astype(BF16)
        rate_here = srecv[m, 0, DV:DV + 1, :]
        absorb(0, qk, val, gate, rate_here)
        made = [gradients(i, srecv[m, 0, 0:DV, :], srecv[m, 1, 0:DV, :], per_chunk, rate_here)
                for i in range(per_chunk)]
        for i in range(per_chunk):
            gsend[m, block_rows(i), :] = made[i][3] * signal_scale
            put(low, block_rows(i), made[i])
        for i in range(per_chunk):
            signal_copy(m, near[m], i).start()

    with jax.named_scope("mix_own"):
        mix(low[...], lambda at: w_s[at, :], None)
    x_chunk.wait()
    for m, o in enumerate(near):
        s = o - 1
        with jax.named_scope(f"whole{m}"):
            if m != 1:
                last_group(s)
            whole(s)
        with jax.named_scope(f"fill{m}"):
            fill(s, m)
        if m == 0:
            for later in order[1:2]:
                last_group(later)
        with jax.named_scope(f"mix{m}"):
            mix(low[...], lambda at: wl[s, at, :].astype(BF16), s == order[-1])
    out_copy = pltpu.make_async_copy(tok_s.at[1, pl.ds(0, mine)], out_hbm, out_sem.at[1])
    out_copy.start()
    with jax.named_scope("end"):
        for m, o in enumerate(near):
            for i in range(per_chunk):
                signal_copy(m, o, i).wait_recv()
        gs_copy = pltpu.make_async_copy(gsb, gs_hbm, out_sem.at[0])
        gs_copy.start()
        for s in order:
            wy_copy(s + 1).wait_send()
            for turn in turns:
                w1_copy(s, turn).wait_send()
                w2_copy(s, turn, 0).wait_send()
                w2_copy(s, turn, 1).wait_send()
                if ring > 2:
                    f1_copy(s, turn).wait_send()
                    f2_copy(s, turn).wait_send()
            for n in range(ring):
                wd_copy(s, n).wait_send()
        for m, o in enumerate(near):
            og_copy(m, o).wait_send()
            state_copy(m, o).wait_send()
            for i in range(per_chunk):
                signal_copy(m, o, i).wait_send()
        out_copy.wait()
        gs_copy.wait()


def per_device(dims, tokens, w_query, w_key, w_value, w_gate, gate_rate, out_grad):
    nx, nz, ny = dims
    rows, width = tokens.shape
    blocks = rows // BT
    mine = rows // ny
    quarter = DV // nz
    whole_tokens = rows * nx * nz * 2
    signal_scale = 4.0 * math.sqrt(whole_tokens * DK / DV)

    count_near = ny - 1
    any_spec = pl.BlockSpec(memory_space=pl.ANY)
    vmem_spec = pl.BlockSpec(memory_space=pltpu.VMEM)
    dma = pltpu.SemaphoreType.DMA
    mixed, signal = pl.pallas_call(
        functools.partial(body, (nx, nz, ny, rows, width, blocks), signal_scale),
        out_shape=(
            jax.ShapeDtypeStruct((mine, width), BF16),
            jax.ShapeDtypeStruct((rows, DK), F32),
        ),
        in_specs=[any_spec] * 5 + [vmem_spec, any_spec],
        out_specs=(any_spec, any_spec),
        scratch_shapes=[
            pltpu.VMEM((width, NW), BF16),
            pltpu.VMEM((2, 2 * BT, width), BF16),
            pltpu.VMEM((rows, DV), BF16),
            pltpu.VMEM((rows, DK), BF16),
            pltpu.VMEM((rows, DK), BF16),
            pltpu.VMEM((rows, DV), BF16),
            pltpu.VMEM((rows, DK), F32),
            pltpu.VMEM((rows, DK), F32),
            pltpu.VMEM((2, BT, BT), BF16),
            pltpu.VMEM((8, DK), F32),
            pltpu.VMEM((blocks + 1, DV, DK), F32),
            pltpu.VMEM((blocks + 1, DV, DK), F32),
            pltpu.VMEM((2, DV + 8, DK), F32),
            pltpu.VMEM((DV + 8, DK), F32),
            pltpu.VMEM((nz, quarter + 8, DK), F32),
            pltpu.VMEM((nz, quarter + 8, DK), F32),
            pltpu.VMEM((nz, quarter + 8, DK), F32),
            pltpu.VMEM((quarter + 8, DK), F32),
            pltpu.VMEM((nx - 1, quarter + 8, DK), F32),
            pltpu.VMEM((nz, quarter, DK), F32),
            pltpu.VMEM((nz, quarter, DK), F32),
            pltpu.VMEM((DV, DK), F32),
            pltpu.VMEM((2, DV, DK), F32),
            pltpu.VMEM((rows, DK), F32),
            pltpu.VMEM((mine, width), F32),
            pltpu.VMEM((width // (nx * nz * 2), NW), F32),
            pltpu.VMEM((ny - 1, width, NW), F32),
            pltpu.VMEM((mine, NW), BF16),
            pltpu.VMEM((count_near, mine, DV), F32),
            pltpu.VMEM((count_near, mine, DV), F32),
            pltpu.VMEM((count_near, 2, DV + 8, DK), F32),
            pltpu.VMEM((count_near, 2, DV + 8, DK), F32),
            pltpu.VMEM((count_near, mine, DK), F32),
            dma((5,)),
            dma((2,)),
            dma((2,)),
            dma((2, nz - 1)),
            dma((2, nx - 1)),
            dma((2, nz - 1)),
            dma((2,)),
            dma((2,)),
            dma((2, ny - 1)),
            dma((2, ny - 1, 2)),
            dma((2, ny - 1, 2)),
            dma((2, ny - 1, 2, 2)),
            dma((2, ny - 1, 2)),
            dma((2, ny - 1, nx)),
            dma((2, count_near)),
            dma((2, count_near)),
            dma((2, count_near, blocks // ny)),
        ],
        compiler_params=pltpu.CompilerParams(
            collective_id=0, has_side_effects=True, vmem_limit_bytes=62 * 2**20),
        cost_estimate=pl.CostEstimate(
            flops=40_000_000_000, bytes_accessed=30_000_000, transcendentals=1_000_000),
    )(tokens, w_query, w_key, w_value, w_gate, gate_rate.reshape(1, DK), out_grad)

    return mixed, signal


def solution(mesh, shape=(4, 4)):
    nx, nz = shape
    ny = mesh.shape["tp"]
    torus = Mesh(mesh.devices.reshape(nx, nz, 2, ny), SEQ_TP)
    placed = (
        P(SEQ, None),
        P(None, "tp"),
        P(None, "tp"),
        P(None, "tp"),
        P(None, "tp"),
        P("tp"),
        P(SEQ, "tp"),
    )
    return jax.shard_map(
        functools.partial(per_device, (nx, nz, ny)),
        mesh=torus,
        in_specs=placed,
        out_specs=(P(SEQ_TP, None), P(SEQ, "tp")),
        check_vma=False,
    )
```

```python
import functools
import math

import jax
import jax.numpy as jnp
from jax import lax
from jax.experimental import pallas as pl
from jax.experimental.pallas import tpu as pltpu
from jax.sharding import Mesh
from jax.sharding import PartitionSpec as P

DK = 128
DV = 256
BT = 256
NW = 3 * DK + DV
SEQ = ("seq_0", "seq_1", "seq_2")
SEQ_TP = ("seq_0", "seq_1", "seq_2", "tp")
MESH = pl.DeviceIdType.MESH
F32 = jnp.float32
BF16 = jnp.bfloat16


def mm(a, b):
    return lax.dot_general(a, b, (((1,), (0,)), ((), ())), preferred_element_type=F32)


def mm_nt(a, b):
    return lax.dot_general(a, b, (((1,), (1,)), ((), ())), preferred_element_type=F32)


def mm_tn(a, b):
    return lax.dot_general(a, b, (((0,), (0,)), ((), ())), preferred_element_type=F32)


def split(a):
    high = a.astype(BF16)
    return high, (a - high.astype(F32)).astype(BF16)


def steps(ny):
    return sorted(range(1, ny), key=lambda o: (-min(o, ny - o), o))


def body(dims, signal_scale, tok_hbm, wq, wk, wv, wg, rate_ref, og_hbm, out_hbm, gs_hbm,
         w_s, tok_s, og_s, qt, kt, vs, cs, sq, tri, carry, spre, gpre, dmsg, dpart, zsend, zrecv, zexc,
         xsend, xrecv, fsend, frecv, psend, states, gsb, acc, wsend, wl,
         low, made, fsw, osend, orecv, ssend, srecv, gsend,
         load_sem, tok_sem, d_sem, z_sem, x_sem, f_sem, p_sem, out_sem,
         wy_sem, w1_sem, f1_sem, w2_sem, f2_sem, wd_sem, og_sem, s_sem, gs_sem, fy_sem):
    nx, nz, ny, rows, width, blocks = dims
    x, z, c, y = (lax.axis_index(a) for a in SEQ_TP)
    sgn = 1 - 2 * c
    per_chunk = blocks // ny
    quarter = DV // nz
    pairs = blocks // 2
    mine = rows // ny
    near = steps(ny)
    order = [o - 1 for o in near]
    direct = order[-1] if nx > 2 and ny > 2 else None

    ring = nx
    share = width // (ring * ring * 2)
    first = x + c * (z - x)
    second = z + c * (x - z)

    def place(a, b):
        return {"seq_0": a + c * (b - a), "seq_1": b + c * (a - b)}

    def wrap(v):
        return lax.rem(v + ring, ring)

    def share_at(a, b, part, parts):
        size = share // parts
        start = ((c * ring + a) * ring + b) * share + part * size
        return pl.ds(pl.multiple_of(start, 8), size)

    def group_at(a, part, parts):
        size = ring * share // parts
        start = (c * ring + a) * ring * share + part * size
        return pl.ds(pl.multiple_of(start, 8), size)

    def remote(src, dst, sems, i, to):
        return pltpu.make_async_remote_copy(
            src, dst, sems.at[(0, *i)], sems.at[(1, *i)], device_id=to, device_id_type=MESH)

    def wy_copy(o):
        dst = wl.at[o - 1, share_at(first, second, 0, 1)]
        return remote(wsend, dst, wy_sem, (o - 1,), {"tp": lax.rem(y + o, ny)})

    turns = (0, 1) if ring > 2 else (0,)

    def w1_copy(s, turn):
        ref = wl.at[s, share_at(first, second, 0, 1)]
        return remote(ref, ref, w1_sem, (s, turn), place(first, wrap(second + 1 - 2 * turn)))

    def f1_copy(s, turn):
        ref = wl.at[s, share_at(first, wrap(second - 1 + 2 * turn), turn, 2)]
        return remote(ref, ref, f1_sem, (s, turn), place(first, wrap(second + 1 - 2 * turn)))

    def w2_copy(s, turn, half):
        ref = wl.at[s, group_at(first, half, 2)]
        return remote(ref, ref, w2_sem, (s, turn, half), place(wrap(first + 1 - 2 * turn), second))

    def f2_copy(s, turn):
        ref = wl.at[s, group_at(wrap(first - 1 + 2 * turn), turn, 2)]
        return remote(ref, ref, f2_sem, (s, turn), place(wrap(first + 1 - 2 * turn), second))

    def fy_copy():
        dst = wl.at[direct, group_at(wrap(first + 2), 0, 1)]
        return remote(fsw, dst, fy_sem, (), {"tp": lax.rem(y + direct + 1, ny)})

    def wd_copy(s, n):
        ref = wl.at[s, group_at(lax.rem(first + n, ring), 0, 1)]
        return remote(ref, ref, wd_sem, (s, n), {"seq_2": 1 - c})

    def start_all(copy, s):
        for turn in turns:
            copy(s, turn).start()

    def arrive_all(copy, s):
        for turn in turns:
            copy(s, turn).wait_recv()

    barrier = pltpu.get_barrier_semaphore()
    xrecv[...] = jnp.zeros_like(xrecv)
    peers = [{"seq_2": 1 - c}]
    peers += [{"seq_0": lax.rem(x + d, nx)} for d in range(1, nx)]
    peers += [{"seq_1": lax.rem(z + d, nz)} for d in range(1, nz)]
    peers += [{"tp": lax.rem(y + d, ny)} for d in range(1, ny)]
    for peer in peers:
        pl.semaphore_signal(barrier, inc=1, device_id=peer, device_id_type=MESH)

    weight_loads = [
        pltpu.make_async_copy(wq, w_s.at[:, pl.ds(0, DK)], load_sem.at[0]),
        pltpu.make_async_copy(wk, w_s.at[:, pl.ds(DK, DK)], load_sem.at[1]),
        pltpu.make_async_copy(wv, w_s.at[:, pl.ds(2 * DK, DV)], load_sem.at[2]),
        pltpu.make_async_copy(wg, w_s.at[:, pl.ds(2 * DK + DV, DK)], load_sem.at[3]),
    ]
    grad_load = pltpu.make_async_copy(og_hbm, og_s, load_sem.at[4])

    def tok_copy(i):
        slot = lax.rem(i, 2)
        start = pl.multiple_of(i * 2 * BT, 2 * BT)
        return pltpu.make_async_copy(tok_hbm.at[pl.ds(start, 2 * BT)], tok_s.at[slot], tok_sem.at[slot])

    def chunk(j):
        return pl.ds(pl.multiple_of(j * mine, mine), mine)

    def block_rows(b):
        return pl.ds(pl.multiple_of(b * BT, BT), BT)

    def og_copy(m, o):
        return remote(osend.at[m], orecv.at[m], og_sem, (m,), {"tp": lax.rem(y + o, ny)})

    def state_copy(m, o):
        return remote(ssend.at[m], srecv.at[m], s_sem, (m,), {"tp": lax.rem(y + o, ny)})

    def signal_copy(m, o, i):
        return remote(gsend.at[m, block_rows(i)], gsb.at[block_rows(y * per_chunk + i)], gs_sem, (m, i),
                      {"tp": lax.rem(y - o + ny, ny)})

    for load in weight_loads:
        load.start()
    tok_copy(0).start()
    grad_load.start()

    at = lax.broadcasted_iota(jnp.int32, (BT, BT), 0)
    before = lax.broadcasted_iota(jnp.int32, (BT, BT), 1)
    tri[0] = (at >= before).astype(F32).astype(BF16)
    tri[1] = (at <= before).astype(F32).astype(BF16)
    carry[...] = jnp.zeros_like(carry)
    spre[0] = jnp.zeros((DV, DK), F32)
    gpre[0] = jnp.zeros((DV, DK), F32)
    rate = rate_ref[...]
    with jax.named_scope("wload"):
        for load in weight_loads:
            load.wait()
    wsend[...] = w_s[share_at(first, second, 0, 1), :].astype(F32)
    with jax.named_scope("barrier"):
        pl.semaphore_wait(barrier, len(peers))
    for s in order:
        wy_copy(s + 1).start()

    def absorb(first_b, qk, val, gate, rate_here):
        count = qk.shape[0] // BT
        parts = [slice(n * BT, (n + 1) * BT) for n in range(count)]
        squashed = [jax.nn.sigmoid(gate[part]) for part in parts]
        pieces = [split(-rate_here * part) for part in squashed]
        running = [mm(tri[0], high) + mm(tri[0], low) for high, low in pieces]
        base = carry[0:1, :]
        for n in range(count):
            running[n] = running[n] + base
            base = running[n][BT - 1:BT, :]
        carry[0:1, :] = base
        q_run = [(qk[parts[n], 0:DK].astype(BF16).astype(F32) * jnp.exp(running[n])).astype(BF16) for n in range(count)]
        k_run = [(qk[parts[n], DK:2 * DK].astype(BF16).astype(F32) * jnp.exp(-running[n])).astype(BF16)
                 for n in range(count)]
        v_here = [val[part].astype(BF16) for part in parts]
        s_terms = [mm_tn(v_here[n], k_run[n]) for n in range(count)]
        g_terms = [mm_tn(og_s[block_rows(first_b + n), :], q_run[n]) for n in range(count)]
        s_sum, g_sum = spre[first_b], gpre[first_b]
        for n in range(count):
            rows_b = block_rows(first_b + n)
            s_sum = s_sum + s_terms[n]
            g_sum = g_sum + g_terms[n]
            sq[rows_b, :] = squashed[n]
            cs[rows_b, :] = running[n]
            qt[rows_b, :] = q_run[n]
            kt[rows_b, :] = k_run[n]
            vs[rows_b, :] = v_here[n]
            spre[first_b + n + 1] = s_sum
            gpre[first_b + n + 1] = g_sum

    def gradients(b, s_in, g_out, last, rate_here):
        rows_b = block_rows(b)
        q_run = qt[rows_b, :]
        k_run = kt[rows_b, :]
        v_here = vs[rows_b, :]
        o_grad = og_s[rows_b, :]
        running = cs[rows_b, :]
        squashed = sq[rows_b, :]
        upper = tri[1].astype(F32)
        lower = tri[0].astype(F32)
        scores_t = (mm_nt(k_run, q_run) * upper).astype(BF16)
        d_scores = (mm_nt(o_grad, v_here) * lower).astype(BF16)
        d_scores_t = (mm_nt(v_here, o_grad) * upper).astype(BF16)
        state = s_in + spre[b]
        after = s_in + spre[b + 1]
        cotangent = g_out + (gpre[last] - gpre[b + 1])
        state_low = state.astype(BF16)
        cot_low = cotangent.astype(BF16)
        dv = mm(scores_t, o_grad) + mm_nt(k_run, cot_low)
        dq = mm(o_grad, state_low) + mm(d_scores, k_run)
        dk = mm(v_here, cot_low) + mm(d_scores_t, q_run)
        boundary = jnp.sum(after * cotangent, axis=0, keepdims=True)
        high, low = split(q_run.astype(F32) * dq - k_run.astype(F32) * dk)
        dg = mm(tri[1], high) + mm(tri[1], low) + boundary
        pre = dg * (-rate_here) * squashed * (1.0 - squashed)
        return dq * jnp.exp(running), dk * jnp.exp(-running), dv, pre

    def put(ref, rows_b, parts):
        dq, dk, dv, pre = parts
        ref[rows_b, 0:DK] = dq.astype(ref.dtype)
        ref[rows_b, DK:2 * DK] = dk.astype(ref.dtype)
        ref[rows_b, 2 * DK:2 * DK + DV] = dv.astype(ref.dtype)
        ref[rows_b, 2 * DK + DV:] = pre.astype(ref.dtype)

    def project(here, weights):
        gate = mm(here, weights(2 * DK + DV, NW))
        return mm(here, weights(0, 2 * DK)), mm(here, weights(2 * DK, 2 * DK + DV)), gate

    def held():
        return made[:, 0:2 * DK], made[:, 2 * DK:2 * DK + DV], made[:, 2 * DK + DV:]

    def hold(parts):
        made[:, 0:2 * DK], made[:, 2 * DK:2 * DK + DV], made[:, 2 * DK + DV:] = parts

    def own_weights(first_col, end_col):
        return w_s[:, first_col:end_col]

    with jax.named_scope("proj"):
        if pairs > 1:
            tok_copy(1).start()
        tok_copy(0).wait()
        hold(project(tok_s[0], own_weights))
        grad_load.wait()

        @pl.loop(1, pairs)
        def _(i):
            @pl.when(i + 1 < pairs)
            def _():
                tok_copy(i + 1).start()

            @pl.when(i == pairs - 1)
            def _():
                if direct is not None:
                    fsw[...] = w_s[group_at(wrap(first + 2), 0, 1), :].astype(F32)
                for m, o in enumerate(near):
                    osend[m] = og_s[chunk(lax.rem(y + o, ny)), :].astype(F32)
                for s in order[:2]:
                    wy_copy(s + 1).wait_recv()
                    start_all(w1_copy, s)
                if direct is not None:
                    fy_copy().start()
                for m, o in enumerate(near[:2]):
                    og_copy(m, o).start()

            tok_copy(i).wait()
            parts = project(tok_s[lax.rem(i, 2)], own_weights)
            absorb(i * 2 - 2, *held(), rate)
            hold(parts)

        for s in order[2:]:
            wy_copy(s + 1).wait_recv()
            start_all(w1_copy, s)
        absorb(blocks - 2, *held(), rate)

    x_chunk = pltpu.make_async_copy(tok_hbm.at[chunk(y)], tok_s.at[0, pl.ds(0, mine)], tok_sem.at[0])
    x_chunk.start()

    def forward_w1(s):
        arrive_all(w1_copy, s)
        if ring > 2:
            start_all(f1_copy, s)

    def start_w2(s, halves=(0, 1)):
        if ring > 2 and 0 in halves:
            arrive_all(f1_copy, s)
        for half in halves:
            for turn in turns:
                w2_copy(s, turn, half).start()

    def arrive_w2(s):
        for half in range(2):
            for turn in turns:
                w2_copy(s, turn, half).wait_recv()

    log_total = carry[0:1, :]
    decay = jnp.exp(log_total)
    dmsg[0, 0:DV, :] = spre[blocks] * decay
    dmsg[1, 0:DV, :] = gpre[blocks]
    for kind in range(2):
        dmsg[kind, DV:DV + 8, :] = jnp.broadcast_to(log_total, (8, DK))

    d_copy = pltpu.make_async_remote_copy(
        dmsg.at[1 - c], dpart, d_sem.at[0], d_sem.at[1], device_id={"seq_2": 1 - c}, device_id_type=MESH)
    with jax.named_scope("d2d"):
        d_copy.start()
        for s in order[:2]:
            forward_w1(s)
        d_copy.wait()

    chip_log = log_total + dpart[DV:DV + 1, :]
    chip = dpart[0:DV, :] + jnp.exp(dpart[DV:DV + 1, :]) * dmsg[c, 0:DV, :]
    for n in range(nz):
        zsend[n, 0:quarter, :] = chip[n * quarter:(n + 1) * quarter, :]
        zsend[n, quarter:quarter + 8, :] = jnp.broadcast_to(chip_log, (8, DK))
    zrecv[z] = zsend[z]
    z_copies = []
    for d in range(1, nz):
        to = lax.rem(z + d, nz)
        z_copies.append(pltpu.make_async_remote_copy(
            zsend.at[to], zrecv.at[z], z_sem.at[0, d - 1], z_sem.at[1, d - 1],
            device_id={"seq_1": to}, device_id_type=MESH))
    for copy in z_copies:
        copy.start()
    with jax.named_scope("w1z"):
        for s in order[2:]:
            forward_w1(s)
        start_w2(order[0])

    with jax.named_scope("zex"):
        for copy in z_copies:
            copy.wait()

    total = jnp.zeros((quarter, DK), F32)
    total_log = jnp.zeros((1, DK), F32)
    for n in range(nz):
        src = c * (nz - 1) + sgn * n
        zexc[src, 0:quarter, :] = total
        zexc[src, quarter:quarter + 8, :] = jnp.broadcast_to(total_log, (8, DK))
        log_here = zrecv[src, quarter:quarter + 1, :]
        total = zrecv[src, 0:quarter, :] + jnp.exp(log_here) * total
        total_log = total_log + log_here
    xsend[0:quarter, :] = total
    xsend[quarter:quarter + 8, :] = jnp.broadcast_to(total_log, (8, DK))

    def x_copy(d):
        to = x + sgn * d
        inside = (to >= 0) & (to < nx)
        return inside, pltpu.make_async_remote_copy(
            xsend, xrecv.at[d - 1], x_sem.at[0, d - 1], x_sem.at[1, d - 1],
            device_id={"seq_0": jnp.where(inside, to, 1 - jnp.minimum(x, 1))}, device_id_type=MESH)

    for d in range(1, nx):
        inside, copy = x_copy(d)
        pl.when(inside)(copy.start)

    for s in order[1:2]:
        start_w2(s, (0,))

    @pl.when(c == 0)
    def _():
        for s in order[1:2]:
            start_w2(s, (1,))

    with jax.named_scope("xex"):
        for d in range(1, nx):
            inside, copy = x_copy(d)
            pl.when(inside)(copy.wait_send)
            source = x - sgn * d
            pl.when((source >= 0) & (source < nx))(copy.wait_recv)

    entering = jnp.zeros((quarter, DK), F32)
    for d in reversed(range(1, nx)):
        entering = xrecv[d - 1, 0:quarter, :] + jnp.exp(xrecv[d - 1, quarter:quarter + 1, :]) * entering
    for n in range(nz):
        fsend[n] = zexc[n, 0:quarter, :] + jnp.exp(zexc[n, quarter:quarter + 1, :]) * entering
    frecv[z] = fsend[z]
    f_copies = []
    for d in range(1, nz):
        to = lax.rem(z + d, nz)
        f_copies.append(pltpu.make_async_remote_copy(
            fsend.at[to], frecv.at[z], f_sem.at[0, d - 1], f_sem.at[1, d - 1],
            device_id={"seq_1": to}, device_id_type=MESH))
    for copy in f_copies:
        copy.start()

    @pl.when(c == 1)
    def _():
        for s in order[1:2]:
            start_w2(s, (1,))

    def forward_w2(s):
        arrive_w2(s)
        if ring > 2 and s != direct:
            start_all(f2_copy, s)

    def group_done(s):
        for n in sorted({0, 1, ring - 1}):
            wd_copy(s, n).start()

    def last_group(s):
        if ring > 2:
            if s == direct:
                fy_copy().wait_recv()
            else:
                arrive_all(f2_copy, s)
            wd_copy(s, 2).start()

    def whole(s):
        for n in range(ring):
            wd_copy(s, n).wait_recv()

    with jax.named_scope("fex"):
        for copy in f_copies:
            copy.wait()
    with jax.named_scope("w2z"):
        forward_w2(order[0])

    entered = frecv[...].reshape(DV, DK)
    psend[...] = dmsg[c, 0:DV, :] + decay * entered
    states[c] = entered
    p_copy = pltpu.make_async_remote_copy(
        psend, states.at[c], p_sem.at[0], p_sem.at[1], device_id={"seq_2": 1 - c}, device_id_type=MESH)
    p_copy.start()
    group_done(order[0])
    with jax.named_scope("pex"):
        p_copy.wait()

    states[1] = states[1] * decay
    for m, o in enumerate(near):
        to = lax.rem(y + o, ny)
        start_log = cs[pl.ds(pl.multiple_of(jnp.maximum(to * mine - 8, 0), 8), 8), :][7:8, :]
        start_log = jnp.where(to > 0, start_log, 0.0)
        ssend[m, 0, 0:DV, :] = (states[0] + spre[to * per_chunk]) * jnp.exp(start_log)
        ssend[m, 1, 0:DV, :] = (states[1] + (gpre[blocks] - gpre[(to + 1) * per_chunk])) * jnp.exp(-start_log)
        ssend[m, 0, DV:DV + 8, :] = jnp.broadcast_to(rate, (8, DK))
        ssend[m, 1, DV:DV + 8, :] = jnp.broadcast_to(rate, (8, DK))

    for m, o in enumerate(near):
        state_copy(m, o).start()

    with jax.named_scope("own"):
        found = [gradients(y * per_chunk + i, states[0], states[1], blocks, rate) for i in range(per_chunk)]
        for i in range(per_chunk):
            gsb[block_rows(y * per_chunk + i), :] = found[i][3] * signal_scale
            put(low, block_rows(i), found[i])
    with jax.named_scope("w2a"):
        for s in order[1:2]:
            forward_w2(s)
            group_done(s)
        for s in order[2:]:
            start_w2(s)
    cols = width // 2

    def mix(grads, weights, last):
        @pl.loop(0, width // cols)
        def _(i):
            at = pl.ds(pl.multiple_of(i * cols, cols), cols)
            term = mm_nt(grads, weights(at))
            if last is None:
                acc[:, at] = term
            elif last:
                out_hbm[:, at] = (acc[:, at] + term).astype(BF16)
            else:
                acc[:, at] = acc[:, at] + term

    def fill(s, m):
        carry[...] = jnp.zeros_like(carry)
        spre[0] = jnp.zeros((DV, DK), F32)
        gpre[0] = jnp.zeros((DV, DK), F32)
        here = tok_s[0, 0:mine, :]
        qk, val, gate = project(here, lambda first_col, end_col: wl[s, :, first_col:end_col].astype(BF16))
        if m == min(1, len(near) - 1):
            with jax.named_scope("w2c"):
                for later in order[2:]:
                    forward_w2(later)
                    group_done(later)
        with jax.named_scope(f"ogw{m}"):
            og_copy(m, near[m]).wait_recv()
        with jax.named_scope(f"stw{m}"):
            state_copy(m, near[m]).wait_recv()
        og_s[0:mine, :] = orecv[m].astype(BF16)
        rate_here = srecv[m, 0, DV:DV + 1, :]
        absorb(0, qk, val, gate, rate_here)
        found = [gradients(i, srecv[m, 0, 0:DV, :], srecv[m, 1, 0:DV, :], per_chunk, rate_here)
                for i in range(per_chunk)]
        for i in range(per_chunk):
            gsend[m, block_rows(i), :] = found[i][3] * signal_scale
            put(low, block_rows(i), found[i])
        for i in range(per_chunk):
            signal_copy(m, near[m], i).start()

    with jax.named_scope("mix_own"):
        mix(low[...], lambda at: w_s[at, :], None)
    for m, o in enumerate(near):
        if m >= 2:
            og_copy(m, o).start()
    if direct is not None:
        last_group(direct)
    x_chunk.wait()
    for m, o in enumerate(near):
        s = o - 1
        with jax.named_scope(f"whole{m}"):
            if m != 1 and s != direct:
                last_group(s)
            whole(s)
        with jax.named_scope(f"fill{m}"):
            fill(s, m)
        if m == 0:
            for later in order[1:2]:
                last_group(later)
        with jax.named_scope(f"mix{m}"):
            mix(low[...], lambda at: wl[s, at, :].astype(BF16), s == order[-1])
    with jax.named_scope("end"):
        for m, o in enumerate(near):
            for i in range(per_chunk):
                signal_copy(m, o, i).wait_recv()
        gs_hbm[...] = gsb[...]
        for s in order:
            wy_copy(s + 1).wait_send()
            for turn in turns:
                w1_copy(s, turn).wait_send()
                w2_copy(s, turn, 0).wait_send()
                w2_copy(s, turn, 1).wait_send()
                if ring > 2:
                    f1_copy(s, turn).wait_send()
                    if s != direct:
                        f2_copy(s, turn).wait_send()
            for n in range(ring):
                wd_copy(s, n).wait_send()
        if direct is not None:
            fy_copy().wait_send()
        for m, o in enumerate(near):
            og_copy(m, o).wait_send()
            state_copy(m, o).wait_send()
            for i in range(per_chunk):
                signal_copy(m, o, i).wait_send()


def per_device(dims, tokens, w_query, w_key, w_value, w_gate, gate_rate, out_grad):
    nx, nz, ny = dims
    rows, width = tokens.shape
    blocks = rows // BT
    mine = rows // ny
    quarter = DV // nz
    whole_tokens = rows * nx * nz * 2
    signal_scale = 4.0 * math.sqrt(whole_tokens * DK / DV)

    count_near = ny - 1
    any_spec = pl.BlockSpec(memory_space=pl.ANY)
    vmem_spec = pl.BlockSpec(memory_space=pltpu.VMEM)
    dma = pltpu.SemaphoreType.DMA
    mixed, signal = pl.pallas_call(
        functools.partial(body, (nx, nz, ny, rows, width, blocks), signal_scale),
        out_shape=(
            pltpu.VMEM((mine, width), BF16),
            pltpu.VMEM((rows, DK), F32),
        ),
        in_specs=[any_spec] * 5 + [vmem_spec, any_spec],
        out_specs=(vmem_spec, vmem_spec),
        scratch_shapes=[
            pltpu.VMEM((width, NW), BF16),
            pltpu.VMEM((2, 2 * BT, width), BF16),
            pltpu.VMEM((rows, DV), BF16),
            pltpu.VMEM((rows, DK), BF16),
            pltpu.VMEM((rows, DK), BF16),
            pltpu.VMEM((rows, DV), BF16),
            pltpu.VMEM((rows, DK), F32),
            pltpu.VMEM((rows, DK), F32),
            pltpu.VMEM((2, BT, BT), BF16),
            pltpu.VMEM((8, DK), F32),
            pltpu.VMEM((blocks + 1, DV, DK), F32),
            pltpu.VMEM((blocks + 1, DV, DK), F32),
            pltpu.VMEM((2, DV + 8, DK), F32),
            pltpu.VMEM((DV + 8, DK), F32),
            pltpu.VMEM((nz, quarter + 8, DK), F32),
            pltpu.VMEM((nz, quarter + 8, DK), F32),
            pltpu.VMEM((nz, quarter + 8, DK), F32),
            pltpu.VMEM((quarter + 8, DK), F32),
            pltpu.VMEM((nx - 1, quarter + 8, DK), F32),
            pltpu.VMEM((nz, quarter, DK), F32),
            pltpu.VMEM((nz, quarter, DK), F32),
            pltpu.VMEM((DV, DK), F32),
            pltpu.VMEM((2, DV, DK), F32),
            pltpu.VMEM((rows, DK), F32),
            pltpu.VMEM((mine, width), F32),
            pltpu.VMEM((width // (nx * nz * 2), NW), F32),
            pltpu.VMEM((ny - 1, width, NW), F32),
            pltpu.VMEM((mine, NW), BF16),
            pltpu.VMEM((2 * BT, NW), F32),
            pltpu.VMEM((width // (2 * nx), NW), F32),
            pltpu.VMEM((count_near, mine, DV), F32),
            pltpu.VMEM((count_near, mine, DV), F32),
            pltpu.VMEM((count_near, 2, DV + 8, DK), F32),
            pltpu.VMEM((count_near, 2, DV + 8, DK), F32),
            pltpu.VMEM((count_near, mine, DK), F32),
            dma((5,)),
            dma((2,)),
            dma((2,)),
            dma((2, nz - 1)),
            dma((2, nx - 1)),
            dma((2, nz - 1)),
            dma((2,)),
            dma((2,)),
            dma((2, ny - 1)),
            dma((2, ny - 1, 2)),
            dma((2, ny - 1, 2)),
            dma((2, ny - 1, 2, 2)),
            dma((2, ny - 1, 2)),
            dma((2, ny - 1, nx)),
            dma((2, count_near)),
            dma((2, count_near)),
            dma((2, count_near, blocks // ny)),
            dma((2,)),
        ],
        compiler_params=pltpu.CompilerParams(
            collective_id=0, has_side_effects=True, vmem_limit_bytes=56 * 2**20),
        cost_estimate=pl.CostEstimate(
            flops=40_000_000_000, bytes_accessed=30_000_000, transcendentals=1_000_000),
    )(tokens, w_query, w_key, w_value, w_gate, gate_rate.reshape(1, DK), out_grad)

    return mixed, signal


def solution(mesh, shape=(4, 4)):
    nx, nz = shape
    ny = mesh.shape["tp"]
    torus = Mesh(mesh.devices.reshape(nx, nz, 2, ny), SEQ_TP)
    placed = (
        P(SEQ, None),
        P(None, "tp"),
        P(None, "tp"),
        P(None, "tp"),
        P(None, "tp"),
        P("tp"),
        P(SEQ, "tp"),
    )
    return jax.shard_map(
        functools.partial(per_device, (nx, nz, ny)),
        mesh=torus,
        in_specs=placed,
        out_specs=(P(SEQ_TP, None), P(SEQ, "tp")),
        check_vma=False,
    )
```

```python
import functools
import math

import jax
import jax.numpy as jnp
from jax import lax
from jax.experimental import pallas as pl
from jax.experimental.pallas import tpu as pltpu
from jax.sharding import Mesh
from jax.sharding import PartitionSpec as P

DK = 128
DV = 256
BT = 256
NW = 3 * DK + DV
SEQ = ("seq_0", "seq_1", "seq_2")
SEQ_TP = ("seq_0", "seq_1", "seq_2", "tp")
MESH = pl.DeviceIdType.MESH
F32 = jnp.float32
BF16 = jnp.bfloat16


def mm(a, b):
    return lax.dot_general(a, b, (((1,), (0,)), ((), ())), preferred_element_type=F32)


def mm_nt(a, b):
    return lax.dot_general(a, b, (((1,), (1,)), ((), ())), preferred_element_type=F32)


def mm_tn(a, b):
    return lax.dot_general(a, b, (((0,), (0,)), ((), ())), preferred_element_type=F32)


def split(a):
    high = a.astype(BF16)
    return high, (a - high.astype(F32)).astype(BF16)


def steps(ny):
    return sorted(range(1, ny), key=lambda o: (-min(o, ny - o), o))


def body(dims, signal_scale, tok_hbm, wq, wk, wv, wg, rate_ref, og_hbm, out_hbm, gs_hbm,
         w_s, tok_s, og_s, qt, kt, vs, cs, sq, tri, carry, spre, gpre, dmsg, dpart, zsend, zrecv, zexc,
         xsend, xrecv, fsend, frecv, psend, states, acc, wsend, wl,
         low, made, fsw, osend, orecv, ssend, srecv,
         load_sem, tok_sem, d_sem, z_sem, x_sem, f_sem, p_sem, out_sem,
         wy_sem, w1_sem, f1_sem, w2_sem, f2_sem, wd_sem, og_sem, s_sem, fy_sem):
    nx, nz, ny, rows, width, blocks = dims
    x, z, c, y = (lax.axis_index(a) for a in SEQ_TP)
    sgn = 1 - 2 * c
    per_chunk = blocks // ny
    quarter = DV // nz
    pairs = blocks // 2
    mine = rows // ny
    near = steps(ny)
    order = [o - 1 for o in near]
    direct = order[-1] if nx > 2 and ny > 2 else None

    ring = nx
    share = width // (ring * ring * 2)
    first = x + c * (z - x)
    second = z + c * (x - z)

    def place(a, b):
        return {"seq_0": a + c * (b - a), "seq_1": b + c * (a - b)}

    def wrap(v):
        return lax.rem(v + ring, ring)

    def share_at(a, b, part, parts):
        size = share // parts
        start = ((c * ring + a) * ring + b) * share + part * size
        return pl.ds(pl.multiple_of(start, 8), size)

    def group_at(a, part, parts):
        size = ring * share // parts
        start = (c * ring + a) * ring * share + part * size
        return pl.ds(pl.multiple_of(start, 8), size)

    def remote(src, dst, sems, i, to):
        return pltpu.make_async_remote_copy(
            src, dst, sems.at[(0, *i)], sems.at[(1, *i)], device_id=to, device_id_type=MESH)

    def wy_copy(o):
        dst = wl.at[o - 1, share_at(first, second, 0, 1)]
        return remote(wsend, dst, wy_sem, (o - 1,), {"tp": lax.rem(y + o, ny)})

    turns = (0, 1) if ring > 2 else (0,)

    def w1_copy(s, turn):
        ref = wl.at[s, share_at(first, second, 0, 1)]
        return remote(ref, ref, w1_sem, (s, turn), place(first, wrap(second + 1 - 2 * turn)))

    def f1_copy(s, turn):
        ref = wl.at[s, share_at(first, wrap(second - 1 + 2 * turn), turn, 2)]
        return remote(ref, ref, f1_sem, (s, turn), place(first, wrap(second + 1 - 2 * turn)))

    def w2_copy(s, turn, half):
        ref = wl.at[s, group_at(first, half, 2)]
        return remote(ref, ref, w2_sem, (s, turn, half), place(wrap(first + 1 - 2 * turn), second))

    def f2_copy(s, turn):
        ref = wl.at[s, group_at(wrap(first - 1 + 2 * turn), turn, 2)]
        return remote(ref, ref, f2_sem, (s, turn), place(wrap(first + 1 - 2 * turn), second))

    def fy_copy():
        dst = wl.at[direct, group_at(wrap(first + 2), 0, 1)]
        return remote(fsw, dst, fy_sem, (), {"tp": lax.rem(y + direct + 1, ny)})

    def wd_copy(s, n):
        ref = wl.at[s, group_at(lax.rem(first + n, ring), 0, 1)]
        return remote(ref, ref, wd_sem, (s, n), {"seq_2": 1 - c})

    def start_all(copy, s):
        for turn in turns:
            copy(s, turn).start()

    def arrive_all(copy, s):
        for turn in turns:
            copy(s, turn).wait_recv()

    barrier = pltpu.get_barrier_semaphore()
    xrecv[...] = jnp.zeros_like(xrecv)
    peers = [{"seq_2": 1 - c}]
    peers += [{"seq_0": lax.rem(x + d, nx)} for d in range(1, nx)]
    peers += [{"seq_1": lax.rem(z + d, nz)} for d in range(1, nz)]
    peers += [{"tp": lax.rem(y + d, ny)} for d in range(1, ny)]
    for peer in peers:
        pl.semaphore_signal(barrier, inc=1, device_id=peer, device_id_type=MESH)

    weight_loads = [
        pltpu.make_async_copy(wq, w_s.at[:, pl.ds(0, DK)], load_sem.at[0]),
        pltpu.make_async_copy(wk, w_s.at[:, pl.ds(DK, DK)], load_sem.at[1]),
        pltpu.make_async_copy(wv, w_s.at[:, pl.ds(2 * DK, DV)], load_sem.at[2]),
        pltpu.make_async_copy(wg, w_s.at[:, pl.ds(2 * DK + DV, DK)], load_sem.at[3]),
    ]
    grad_load = pltpu.make_async_copy(og_hbm, og_s, load_sem.at[4])

    def tok_copy(i):
        slot = lax.rem(i, 2)
        start = pl.multiple_of(i * 2 * BT, 2 * BT)
        return pltpu.make_async_copy(tok_hbm.at[pl.ds(start, 2 * BT)], tok_s.at[slot], tok_sem.at[slot])

    def chunk(j):
        return pl.ds(pl.multiple_of(j * mine, mine), mine)

    def block_rows(b):
        return pl.ds(pl.multiple_of(b * BT, BT), BT)

    def og_copy(m, o):
        return remote(osend.at[m], orecv.at[m], og_sem, (m,), {"tp": lax.rem(y + o, ny)})

    def state_copy(m, o):
        return remote(ssend.at[m], srecv.at[m], s_sem, (m,), {"tp": lax.rem(y + o, ny)})

    for load in weight_loads:
        load.start()
    tok_copy(0).start()
    grad_load.start()

    at = lax.broadcasted_iota(jnp.int32, (BT, BT), 0)
    before = lax.broadcasted_iota(jnp.int32, (BT, BT), 1)
    tri[0] = (at >= before).astype(F32).astype(BF16)
    tri[1] = (at <= before).astype(F32).astype(BF16)
    carry[...] = jnp.zeros_like(carry)
    spre[0] = jnp.zeros((DV, DK), F32)
    gpre[0] = jnp.zeros((DV, DK), F32)
    rate = rate_ref[...]
    with jax.named_scope("wload"):
        for load in weight_loads:
            load.wait()
    wsend[...] = w_s[share_at(first, second, 0, 1), :].astype(F32)
    with jax.named_scope("barrier"):
        pl.semaphore_wait(barrier, len(peers))
    for s in order:
        wy_copy(s + 1).start()

    def absorb(first_b, qk, val, gate, rate_here):
        count = qk.shape[0] // BT
        parts = [slice(n * BT, (n + 1) * BT) for n in range(count)]
        squashed = [jax.nn.sigmoid(gate[part]) for part in parts]
        pieces = [split(-rate_here * part) for part in squashed]
        running = [mm(tri[0], high) + mm(tri[0], low) for high, low in pieces]
        base = carry[0:1, :]
        for n in range(count):
            running[n] = running[n] + base
            base = running[n][BT - 1:BT, :]
        carry[0:1, :] = base
        q_run = [(qk[parts[n], 0:DK].astype(BF16).astype(F32) * jnp.exp(running[n])).astype(BF16) for n in range(count)]
        k_run = [(qk[parts[n], DK:2 * DK].astype(BF16).astype(F32) * jnp.exp(-running[n])).astype(BF16)
                 for n in range(count)]
        v_here = [val[part].astype(BF16) for part in parts]
        s_terms = [mm_tn(v_here[n], k_run[n]) for n in range(count)]
        g_terms = [mm_tn(og_s[block_rows(first_b + n), :], q_run[n]) for n in range(count)]
        s_sum, g_sum = spre[first_b], gpre[first_b]
        for n in range(count):
            rows_b = block_rows(first_b + n)
            s_sum = s_sum + s_terms[n]
            g_sum = g_sum + g_terms[n]
            sq[rows_b, :] = squashed[n]
            cs[rows_b, :] = running[n]
            qt[rows_b, :] = q_run[n]
            kt[rows_b, :] = k_run[n]
            vs[rows_b, :] = v_here[n]
            spre[first_b + n + 1] = s_sum
            gpre[first_b + n + 1] = g_sum

    def gradients(b, s_in, g_out, last, rate_here):
        rows_b = block_rows(b)
        q_run = qt[rows_b, :]
        k_run = kt[rows_b, :]
        v_here = vs[rows_b, :]
        o_grad = og_s[rows_b, :]
        running = cs[rows_b, :]
        squashed = sq[rows_b, :]
        upper = tri[1].astype(F32)
        lower = tri[0].astype(F32)
        scores_t = (mm_nt(k_run, q_run) * upper).astype(BF16)
        d_scores = (mm_nt(o_grad, v_here) * lower).astype(BF16)
        d_scores_t = (mm_nt(v_here, o_grad) * upper).astype(BF16)
        state = s_in + spre[b]
        after = s_in + spre[b + 1]
        cotangent = g_out + (gpre[last] - gpre[b + 1])
        state_low = state.astype(BF16)
        cot_low = cotangent.astype(BF16)
        dv = mm(scores_t, o_grad) + mm_nt(k_run, cot_low)
        dq = mm(o_grad, state_low) + mm(d_scores, k_run)
        dk = mm(v_here, cot_low) + mm(d_scores_t, q_run)
        boundary = jnp.sum(after * cotangent, axis=0, keepdims=True)
        high, low = split(q_run.astype(F32) * dq - k_run.astype(F32) * dk)
        dg = mm(tri[1], high) + mm(tri[1], low) + boundary
        pre = dg * (-rate_here) * squashed * (1.0 - squashed)
        return dq * jnp.exp(running), dk * jnp.exp(-running), dv, pre

    def put(ref, rows_b, parts):
        dq, dk, dv, pre = parts
        ref[rows_b, 0:DK] = dq.astype(ref.dtype)
        ref[rows_b, DK:2 * DK] = dk.astype(ref.dtype)
        ref[rows_b, 2 * DK:2 * DK + DV] = dv.astype(ref.dtype)
        ref[rows_b, 2 * DK + DV:] = pre.astype(ref.dtype)

    def project(here, weights):
        gate = mm(here, weights(2 * DK + DV, NW))
        return mm(here, weights(0, 2 * DK)), mm(here, weights(2 * DK, 2 * DK + DV)), gate

    def held():
        return made[:, 0:2 * DK], made[:, 2 * DK:2 * DK + DV], made[:, 2 * DK + DV:]

    def hold(parts):
        made[:, 0:2 * DK], made[:, 2 * DK:2 * DK + DV], made[:, 2 * DK + DV:] = parts

    def own_weights(first_col, end_col):
        return w_s[:, first_col:end_col]

    with jax.named_scope("proj"):
        if pairs > 1:
            tok_copy(1).start()
        tok_copy(0).wait()
        hold(project(tok_s[0], own_weights))
        grad_load.wait()

        @pl.loop(1, pairs)
        def _(i):
            @pl.when(i + 1 < pairs)
            def _():
                tok_copy(i + 1).start()

            @pl.when(i == pairs - 1)
            def _():
                if direct is not None:
                    fsw[...] = w_s[group_at(wrap(first + 2), 0, 1), :].astype(F32)
                for m, o in enumerate(near):
                    osend[m] = og_s[chunk(lax.rem(y + o, ny)), :].astype(F32)
                for s in order[:2]:
                    wy_copy(s + 1).wait_recv()
                    start_all(w1_copy, s)
                if direct is not None:
                    fy_copy().start()
                for m, o in enumerate(near[:2]):
                    og_copy(m, o).start()

            tok_copy(i).wait()
            parts = project(tok_s[lax.rem(i, 2)], own_weights)
            absorb(i * 2 - 2, *held(), rate)
            hold(parts)

        for s in order[2:]:
            wy_copy(s + 1).wait_recv()
            start_all(w1_copy, s)
        absorb(blocks - 2, *held(), rate)

    x_chunk = pltpu.make_async_copy(tok_hbm.at[chunk(y)], tok_s.at[0, pl.ds(0, mine)], tok_sem.at[0])
    x_chunk.start()

    def forward_w1(s):
        arrive_all(w1_copy, s)
        if ring > 2:
            start_all(f1_copy, s)

    def start_w2(s, halves=(0, 1)):
        if ring > 2 and 0 in halves:
            arrive_all(f1_copy, s)
        for half in halves:
            for turn in turns:
                w2_copy(s, turn, half).start()

    def arrive_w2(s):
        for half in range(2):
            for turn in turns:
                w2_copy(s, turn, half).wait_recv()

    log_total = carry[0:1, :]
    decay = jnp.exp(log_total)
    dmsg[0, 0:DV, :] = spre[blocks] * decay
    dmsg[1, 0:DV, :] = gpre[blocks]
    for kind in range(2):
        dmsg[kind, DV:DV + 8, :] = jnp.broadcast_to(log_total, (8, DK))

    d_copy = pltpu.make_async_remote_copy(
        dmsg.at[1 - c], dpart, d_sem.at[0], d_sem.at[1], device_id={"seq_2": 1 - c}, device_id_type=MESH)
    with jax.named_scope("d2d"):
        d_copy.start()
        for s in order[:2]:
            forward_w1(s)
        d_copy.wait()

    chip_log = log_total + dpart[DV:DV + 1, :]
    chip = dpart[0:DV, :] + jnp.exp(dpart[DV:DV + 1, :]) * dmsg[c, 0:DV, :]
    for n in range(nz):
        zsend[n, 0:quarter, :] = chip[n * quarter:(n + 1) * quarter, :]
        zsend[n, quarter:quarter + 8, :] = jnp.broadcast_to(chip_log, (8, DK))
    zrecv[z] = zsend[z]
    z_copies = []
    for d in range(1, nz):
        to = lax.rem(z + d, nz)
        z_copies.append(pltpu.make_async_remote_copy(
            zsend.at[to], zrecv.at[z], z_sem.at[0, d - 1], z_sem.at[1, d - 1],
            device_id={"seq_1": to}, device_id_type=MESH))
    for copy in z_copies:
        copy.start()
    with jax.named_scope("w1z"):
        for s in order[2:]:
            forward_w1(s)
        start_w2(order[0])

    with jax.named_scope("zex"):
        for copy in z_copies:
            copy.wait()

    total = jnp.zeros((quarter, DK), F32)
    total_log = jnp.zeros((1, DK), F32)
    for n in range(nz):
        src = c * (nz - 1) + sgn * n
        zexc[src, 0:quarter, :] = total
        zexc[src, quarter:quarter + 8, :] = jnp.broadcast_to(total_log, (8, DK))
        log_here = zrecv[src, quarter:quarter + 1, :]
        total = zrecv[src, 0:quarter, :] + jnp.exp(log_here) * total
        total_log = total_log + log_here
    xsend[0:quarter, :] = total
    xsend[quarter:quarter + 8, :] = jnp.broadcast_to(total_log, (8, DK))

    def x_copy(d):
        to = x + sgn * d
        inside = (to >= 0) & (to < nx)
        return inside, pltpu.make_async_remote_copy(
            xsend, xrecv.at[d - 1], x_sem.at[0, d - 1], x_sem.at[1, d - 1],
            device_id={"seq_0": jnp.where(inside, to, 1 - jnp.minimum(x, 1))}, device_id_type=MESH)

    for d in range(1, nx):
        inside, copy = x_copy(d)
        pl.when(inside)(copy.start)

    for s in order[1:2]:
        start_w2(s, (0,))

    @pl.when(c == 0)
    def _():
        for s in order[1:2]:
            start_w2(s, (1,))

    with jax.named_scope("xex"):
        for d in range(1, nx):
            inside, copy = x_copy(d)
            pl.when(inside)(copy.wait_send)
            source = x - sgn * d
            pl.when((source >= 0) & (source < nx))(copy.wait_recv)

    entering = jnp.zeros((quarter, DK), F32)
    for d in reversed(range(1, nx)):
        entering = xrecv[d - 1, 0:quarter, :] + jnp.exp(xrecv[d - 1, quarter:quarter + 1, :]) * entering
    for n in range(nz):
        fsend[n] = zexc[n, 0:quarter, :] + jnp.exp(zexc[n, quarter:quarter + 1, :]) * entering
    frecv[z] = fsend[z]
    f_copies = []
    for d in range(1, nz):
        to = lax.rem(z + d, nz)
        f_copies.append(pltpu.make_async_remote_copy(
            fsend.at[to], frecv.at[z], f_sem.at[0, d - 1], f_sem.at[1, d - 1],
            device_id={"seq_1": to}, device_id_type=MESH))
    for copy in f_copies:
        copy.start()

    @pl.when(c == 1)
    def _():
        for s in order[1:2]:
            start_w2(s, (1,))

    def forward_w2(s):
        arrive_w2(s)
        if ring > 2 and s != direct:
            start_all(f2_copy, s)

    def group_done(s):
        for n in sorted({0, 1, ring - 1}):
            wd_copy(s, n).start()

    def last_group(s):
        if ring > 2:
            if s == direct:
                fy_copy().wait_recv()
            else:
                arrive_all(f2_copy, s)
            wd_copy(s, 2).start()

    def whole(s):
        for n in range(ring):
            wd_copy(s, n).wait_recv()

    with jax.named_scope("fex"):
        for copy in f_copies:
            copy.wait()
    with jax.named_scope("w2z"):
        forward_w2(order[0])

    entered = frecv[...].reshape(DV, DK)
    psend[...] = dmsg[c, 0:DV, :] + decay * entered
    states[c] = entered
    p_copy = pltpu.make_async_remote_copy(
        psend, states.at[c], p_sem.at[0], p_sem.at[1], device_id={"seq_2": 1 - c}, device_id_type=MESH)
    p_copy.start()
    group_done(order[0])
    with jax.named_scope("pex"):
        p_copy.wait()

    states[1] = states[1] * decay
    for m, o in enumerate(near):
        to = lax.rem(y + o, ny)
        start_log = cs[pl.ds(pl.multiple_of(jnp.maximum(to * mine - 8, 0), 8), 8), :][7:8, :]
        start_log = jnp.where(to > 0, start_log, 0.0)
        ssend[m, 0, 0:DV, :] = (states[0] + spre[to * per_chunk]) * jnp.exp(start_log)
        ssend[m, 1, 0:DV, :] = (states[1] + (gpre[blocks] - gpre[(to + 1) * per_chunk])) * jnp.exp(-start_log)
        ssend[m, 0, DV:DV + 8, :] = jnp.broadcast_to(rate, (8, DK))
        ssend[m, 1, DV:DV + 8, :] = jnp.broadcast_to(rate, (8, DK))

    for m, o in enumerate(near):
        state_copy(m, o).start()

    with jax.named_scope("own"):
        found = [gradients(y * per_chunk + i, states[0], states[1], blocks, rate) for i in range(per_chunk)]
        for i in range(per_chunk):
            gs_hbm[block_rows(y * per_chunk + i), :] = found[i][3] * signal_scale
            put(low, block_rows(i), found[i])
    cols = width // 2

    def mix(grads, weights, last):
        @pl.loop(0, width // cols)
        def _(i):
            at = pl.ds(pl.multiple_of(i * cols, cols), cols)
            term = mm_nt(grads, weights(at))
            if last is None:
                acc[:, at] = term
            elif last:
                out_hbm[:, at] = (acc[:, at] + term).astype(BF16)
            else:
                acc[:, at] = acc[:, at] + term

    def fill(s, m):
        carry[...] = jnp.zeros_like(carry)
        spre[0] = jnp.zeros((DV, DK), F32)
        gpre[0] = jnp.zeros((DV, DK), F32)
        here = tok_s[0, 0:mine, :]
        qk, val, gate = project(here, lambda first_col, end_col: wl[s, :, first_col:end_col].astype(BF16))
        if m == min(1, len(near) - 1):
            with jax.named_scope("w2c"):
                for later in order[2:]:
                    forward_w2(later)
                    group_done(later)
        with jax.named_scope(f"ogw{m}"):
            og_copy(m, near[m]).wait_recv()
        with jax.named_scope(f"stw{m}"):
            state_copy(m, near[m]).wait_recv()
        og_s[0:mine, :] = orecv[m].astype(BF16)
        rate_here = srecv[m, 0, DV:DV + 1, :]
        absorb(0, qk, val, gate, rate_here)
        found = [gradients(i, srecv[m, 0, 0:DV, :], srecv[m, 1, 0:DV, :], per_chunk, rate_here)
                for i in range(per_chunk)]
        for i in range(per_chunk):
            put(low, block_rows(i), found[i])

    with jax.named_scope("mix_own"):
        mix(low[...], lambda at: w_s[at, :], None)
    with jax.named_scope("w2a"):
        for s in order[1:2]:
            forward_w2(s)
            group_done(s)
        for s in order[2:]:
            start_w2(s)
    with jax.named_scope("signals"):
        @pl.loop(1, ny)
        def _(n):
            @pl.when(n == ny - 1)
            def _():
                last_group(order[0])

            first_b = lax.rem(y + n, ny) * per_chunk
            found = [gradients(first_b + i, states[0], states[1], blocks, rate)[3] for i in range(per_chunk)]
            for i in range(per_chunk):
                gs_hbm[block_rows(first_b + i), :] = found[i] * signal_scale

    for m, o in enumerate(near):
        if m >= 2:
            og_copy(m, o).start()
    if direct is not None:
        last_group(direct)
    x_chunk.wait()
    for m, o in enumerate(near):
        s = o - 1
        with jax.named_scope(f"whole{m}"):
            if m > 1 and s != direct:
                last_group(s)
            whole(s)
        with jax.named_scope(f"fill{m}"):
            fill(s, m)
        if m == 0:
            for later in order[1:2]:
                last_group(later)
        with jax.named_scope(f"mix{m}"):
            mix(low[...], lambda at: wl[s, at, :].astype(BF16), s == order[-1])
    with jax.named_scope("end"):
        for s in order:
            wy_copy(s + 1).wait_send()
            for turn in turns:
                w1_copy(s, turn).wait_send()
                w2_copy(s, turn, 0).wait_send()
                w2_copy(s, turn, 1).wait_send()
                if ring > 2:
                    f1_copy(s, turn).wait_send()
                    if s != direct:
                        f2_copy(s, turn).wait_send()
            for n in range(ring):
                wd_copy(s, n).wait_send()
        if direct is not None:
            fy_copy().wait_send()
        for m, o in enumerate(near):
            og_copy(m, o).wait_send()
            state_copy(m, o).wait_send()


def per_device(dims, tokens, w_query, w_key, w_value, w_gate, gate_rate, out_grad):
    nx, nz, ny = dims
    rows, width = tokens.shape
    blocks = rows // BT
    mine = rows // ny
    quarter = DV // nz
    whole_tokens = rows * nx * nz * 2
    signal_scale = 4.0 * math.sqrt(whole_tokens * DK / DV)

    count_near = ny - 1
    any_spec = pl.BlockSpec(memory_space=pl.ANY)
    vmem_spec = pl.BlockSpec(memory_space=pltpu.VMEM)
    dma = pltpu.SemaphoreType.DMA
    mixed, signal = pl.pallas_call(
        functools.partial(body, (nx, nz, ny, rows, width, blocks), signal_scale),
        out_shape=(
            pltpu.VMEM((mine, width), BF16),
            pltpu.VMEM((rows, DK), F32),
        ),
        in_specs=[any_spec] * 5 + [vmem_spec, any_spec],
        out_specs=(vmem_spec, vmem_spec),
        scratch_shapes=[
            pltpu.VMEM((width, NW), BF16),
            pltpu.VMEM((2, 2 * BT, width), BF16),
            pltpu.VMEM((rows, DV), BF16),
            pltpu.VMEM((rows, DK), BF16),
            pltpu.VMEM((rows, DK), BF16),
            pltpu.VMEM((rows, DV), BF16),
            pltpu.VMEM((rows, DK), F32),
            pltpu.VMEM((rows, DK), F32),
            pltpu.VMEM((2, BT, BT), BF16),
            pltpu.VMEM((8, DK), F32),
            pltpu.VMEM((blocks + 1, DV, DK), F32),
            pltpu.VMEM((blocks + 1, DV, DK), F32),
            pltpu.VMEM((2, DV + 8, DK), F32),
            pltpu.VMEM((DV + 8, DK), F32),
            pltpu.VMEM((nz, quarter + 8, DK), F32),
            pltpu.VMEM((nz, quarter + 8, DK), F32),
            pltpu.VMEM((nz, quarter + 8, DK), F32),
            pltpu.VMEM((quarter + 8, DK), F32),
            pltpu.VMEM((nx - 1, quarter + 8, DK), F32),
            pltpu.VMEM((nz, quarter, DK), F32),
            pltpu.VMEM((nz, quarter, DK), F32),
            pltpu.VMEM((DV, DK), F32),
            pltpu.VMEM((2, DV, DK), F32),
            pltpu.VMEM((mine, width), F32),
            pltpu.VMEM((width // (nx * nz * 2), NW), F32),
            pltpu.VMEM((ny - 1, width, NW), F32),
            pltpu.VMEM((mine, NW), BF16),
            pltpu.VMEM((2 * BT, NW), F32),
            pltpu.VMEM((width // (2 * nx), NW), F32),
            pltpu.VMEM((count_near, mine, DV), F32),
            pltpu.VMEM((count_near, mine, DV), F32),
            pltpu.VMEM((count_near, 2, DV + 8, DK), F32),
            pltpu.VMEM((count_near, 2, DV + 8, DK), F32),
            dma((5,)),
            dma((2,)),
            dma((2,)),
            dma((2, nz - 1)),
            dma((2, nx - 1)),
            dma((2, nz - 1)),
            dma((2,)),
            dma((2,)),
            dma((2, ny - 1)),
            dma((2, ny - 1, 2)),
            dma((2, ny - 1, 2)),
            dma((2, ny - 1, 2, 2)),
            dma((2, ny - 1, 2)),
            dma((2, ny - 1, nx)),
            dma((2, count_near)),
            dma((2, count_near)),
            dma((2,)),
        ],
        compiler_params=pltpu.CompilerParams(
            collective_id=0, has_side_effects=True, vmem_limit_bytes=56 * 2**20),
        cost_estimate=pl.CostEstimate(
            flops=40_000_000_000, bytes_accessed=30_000_000, transcendentals=1_000_000),
    )(tokens, w_query, w_key, w_value, w_gate, gate_rate.reshape(1, DK), out_grad)

    return mixed, signal


def solution(mesh, shape=(4, 4)):
    nx, nz = shape
    ny = mesh.shape["tp"]
    torus = Mesh(mesh.devices.reshape(nx, nz, 2, ny), SEQ_TP)
    placed = (
        P(SEQ, None),
        P(None, "tp"),
        P(None, "tp"),
        P(None, "tp"),
        P(None, "tp"),
        P("tp"),
        P(SEQ, "tp"),
    )
    return jax.shard_map(
        functools.partial(per_device, (nx, nz, ny)),
        mesh=torus,
        in_specs=placed,
        out_specs=(P(SEQ_TP, None), P(SEQ, "tp")),
        check_vma=False,
    )
```

```python
import functools
import math

import jax
import jax.numpy as jnp
from jax import lax
from jax.experimental import pallas as pl
from jax.experimental.pallas import tpu as pltpu
from jax.sharding import Mesh
from jax.sharding import PartitionSpec as P

DK = 128
DV = 256
BT = 256
NW = 3 * DK + DV
SEQ = ("seq_0", "seq_1", "seq_2")
SEQ_TP = ("seq_0", "seq_1", "seq_2", "tp")
MESH = pl.DeviceIdType.MESH
F32 = jnp.float32
BF16 = jnp.bfloat16


def mm(a, b):
    return lax.dot_general(a, b, (((1,), (0,)), ((), ())), preferred_element_type=F32)


def mm_nt(a, b):
    return lax.dot_general(a, b, (((1,), (1,)), ((), ())), preferred_element_type=F32)


def mm_tn(a, b):
    return lax.dot_general(a, b, (((0,), (0,)), ((), ())), preferred_element_type=F32)


def split(a):
    high = a.astype(BF16)
    return high, (a - high.astype(F32)).astype(BF16)


def steps(ny):
    return sorted(range(1, ny), key=lambda o: (-min(o, ny - o), o))


def body(dims, signal_scale, tok_hbm, wq, wk, wv, wg, rate_ref, og_hbm, out_hbm, gs_hbm,
         w_s, tok_s, og_s, qt, kt, vs, cs, sq, tri, carry, spre, gpre, dmsg, dpart, zsend, zrecv, zexc,
         xsend, xrecv, fsend, frecv, psend, states, acc, wsend, wl,
         low, made, fsw, osend, orecv, ssend, srecv,
         load_sem, tok_sem, d_sem, z_sem, x_sem, f_sem, p_sem, out_sem,
         wy_sem, w1_sem, f1_sem, w2_sem, f2_sem, wd_sem, og_sem, s_sem, fy_sem):
    nx, nz, ny, rows, width, blocks = dims
    x, z, c, y = (lax.axis_index(a) for a in SEQ_TP)
    sgn = 1 - 2 * c
    per_chunk = blocks // ny
    quarter = DV // nz
    pairs = blocks // 2
    mine = rows // ny
    near = steps(ny)
    order = [o - 1 for o in near]
    direct = order[-1] if nx > 2 and ny > 2 else None

    ring = nx
    share = width // (ring * ring * 2)
    first = x + c * (z - x)
    second = z + c * (x - z)

    def place(a, b):
        return {"seq_0": a + c * (b - a), "seq_1": b + c * (a - b)}

    def wrap(v):
        return lax.rem(v + ring, ring)

    def share_at(a, b, part, parts):
        size = share // parts
        start = ((c * ring + a) * ring + b) * share + part * size
        return pl.ds(pl.multiple_of(start, 8), size)

    def group_at(a, part, parts):
        size = ring * share // parts
        start = (c * ring + a) * ring * share + part * size
        return pl.ds(pl.multiple_of(start, 8), size)

    def remote(src, dst, sems, i, to):
        return pltpu.make_async_remote_copy(
            src, dst, sems.at[(0, *i)], sems.at[(1, *i)], device_id=to, device_id_type=MESH)

    def wy_copy(o):
        dst = wl.at[o - 1, share_at(first, second, 0, 1)]
        return remote(wsend, dst, wy_sem, (o - 1,), {"tp": lax.rem(y + o, ny)})

    turns = (0, 1) if ring > 2 else (0,)

    def w1_copy(s, turn):
        ref = wl.at[s, share_at(first, second, 0, 1)]
        return remote(ref, ref, w1_sem, (s, turn), place(first, wrap(second + 1 - 2 * turn)))

    def f1_copy(s, turn):
        ref = wl.at[s, share_at(first, wrap(second - 1 + 2 * turn), turn, 2)]
        return remote(ref, ref, f1_sem, (s, turn), place(first, wrap(second + 1 - 2 * turn)))

    def w2_copy(s, turn, half):
        ref = wl.at[s, group_at(first, half, 2)]
        return remote(ref, ref, w2_sem, (s, turn, half), place(wrap(first + 1 - 2 * turn), second))

    def f2_copy(s, turn):
        ref = wl.at[s, group_at(wrap(first - 1 + 2 * turn), turn, 2)]
        return remote(ref, ref, f2_sem, (s, turn), place(wrap(first + 1 - 2 * turn), second))

    def fy_copy():
        dst = wl.at[direct, group_at(wrap(first + 2), 0, 1)]
        return remote(fsw, dst, fy_sem, (), {"tp": lax.rem(y + direct + 1, ny)})

    def wd_copy(s, n):
        ref = wl.at[s, group_at(lax.rem(first + n, ring), 0, 1)]
        return remote(ref, ref, wd_sem, (s, n), {"seq_2": 1 - c})

    def start_all(copy, s):
        for turn in turns:
            copy(s, turn).start()

    def arrive_all(copy, s):
        for turn in turns:
            copy(s, turn).wait_recv()

    barrier = pltpu.get_barrier_semaphore()
    xrecv[...] = jnp.zeros_like(xrecv)
    peers = [{"seq_2": 1 - c}]
    peers += [{"seq_0": lax.rem(x + d, nx)} for d in range(1, nx)]
    peers += [{"seq_1": lax.rem(z + d, nz)} for d in range(1, nz)]
    peers += [{"tp": lax.rem(y + d, ny)} for d in range(1, ny)]
    for peer in peers:
        pl.semaphore_signal(barrier, inc=1, device_id=peer, device_id_type=MESH)

    weight_loads = [
        pltpu.make_async_copy(wq, w_s.at[:, pl.ds(0, DK)], load_sem.at[0]),
        pltpu.make_async_copy(wk, w_s.at[:, pl.ds(DK, DK)], load_sem.at[1]),
        pltpu.make_async_copy(wv, w_s.at[:, pl.ds(2 * DK, DV)], load_sem.at[2]),
        pltpu.make_async_copy(wg, w_s.at[:, pl.ds(2 * DK + DV, DK)], load_sem.at[3]),
    ]
    grad_load = pltpu.make_async_copy(og_hbm, og_s, load_sem.at[4])

    def tok_copy(i):
        slot = lax.rem(i, 2)
        start = pl.multiple_of(i * 2 * BT, 2 * BT)
        return pltpu.make_async_copy(tok_hbm.at[pl.ds(start, 2 * BT)], tok_s.at[slot], tok_sem.at[slot])

    def chunk(j):
        return pl.ds(pl.multiple_of(j * mine, mine), mine)

    def block_rows(b):
        return pl.ds(pl.multiple_of(b * BT, BT), BT)

    def og_copy(m, o):
        return remote(osend.at[m], orecv.at[m], og_sem, (m,), {"tp": lax.rem(y + o, ny)})

    def state_copy(m, o):
        return remote(ssend.at[m], srecv.at[m], s_sem, (m,), {"tp": lax.rem(y + o, ny)})

    for load in weight_loads:
        load.start()
    tok_copy(0).start()
    grad_load.start()

    at = lax.broadcasted_iota(jnp.int32, (BT, BT), 0)
    before = lax.broadcasted_iota(jnp.int32, (BT, BT), 1)
    tri[0] = (at >= before).astype(F32).astype(BF16)
    tri[1] = (at <= before).astype(F32).astype(BF16)
    carry[...] = jnp.zeros_like(carry)
    spre[0] = jnp.zeros((DV, DK), F32)
    gpre[0] = jnp.zeros((DV, DK), F32)
    rate = rate_ref[...]
    with jax.named_scope("wload"):
        for load in weight_loads:
            load.wait()
    wsend[...] = w_s[share_at(first, second, 0, 1), :].astype(F32)
    with jax.named_scope("barrier"):
        pl.semaphore_wait(barrier, len(peers))
    for s in order:
        wy_copy(s + 1).start()

    def absorb(first_b, qk, val, gate, rate_here):
        count = qk.shape[0] // BT
        parts = [slice(n * BT, (n + 1) * BT) for n in range(count)]
        squashed = [jax.nn.sigmoid(gate[part]) for part in parts]
        pieces = [split(-rate_here * part) for part in squashed]
        running = [mm(tri[0], high) + mm(tri[0], low) for high, low in pieces]
        base = carry[0:1, :]
        for n in range(count):
            running[n] = running[n] + base
            base = running[n][BT - 1:BT, :]
        carry[0:1, :] = base
        q_run = [(qk[parts[n], 0:DK].astype(BF16).astype(F32) * jnp.exp(running[n])).astype(BF16) for n in range(count)]
        k_run = [(qk[parts[n], DK:2 * DK].astype(BF16).astype(F32) * jnp.exp(-running[n])).astype(BF16)
                 for n in range(count)]
        v_here = [val[part].astype(BF16) for part in parts]
        s_terms = [mm_tn(v_here[n], k_run[n]) for n in range(count)]
        g_terms = [mm_tn(og_s[block_rows(first_b + n), :], q_run[n]) for n in range(count)]
        s_sum, g_sum = spre[first_b], gpre[first_b]
        for n in range(count):
            rows_b = block_rows(first_b + n)
            s_sum = s_sum + s_terms[n]
            g_sum = g_sum + g_terms[n]
            sq[rows_b, :] = squashed[n]
            cs[rows_b, :] = running[n]
            qt[rows_b, :] = q_run[n]
            kt[rows_b, :] = k_run[n]
            vs[rows_b, :] = v_here[n]
            spre[first_b + n + 1] = s_sum
            gpre[first_b + n + 1] = g_sum

    def gradients(b, s_in, g_out, last, rate_here):
        rows_b = block_rows(b)
        q_run = qt[rows_b, :]
        k_run = kt[rows_b, :]
        v_here = vs[rows_b, :]
        o_grad = og_s[rows_b, :]
        running = cs[rows_b, :]
        squashed = sq[rows_b, :]
        upper = tri[1].astype(F32)
        lower = tri[0].astype(F32)
        scores_t = (mm_nt(k_run, q_run) * upper).astype(BF16)
        d_scores = (mm_nt(o_grad, v_here) * lower).astype(BF16)
        d_scores_t = (mm_nt(v_here, o_grad) * upper).astype(BF16)
        state = s_in + spre[b]
        after = s_in + spre[b + 1]
        cotangent = g_out + (gpre[last] - gpre[b + 1])
        state_low = state.astype(BF16)
        cot_low = cotangent.astype(BF16)
        dv = mm(scores_t, o_grad) + mm_nt(k_run, cot_low)
        dq = mm(o_grad, state_low) + mm(d_scores, k_run)
        dk = mm(v_here, cot_low) + mm(d_scores_t, q_run)
        boundary = jnp.sum(after * cotangent, axis=0, keepdims=True)
        high, low = split(q_run.astype(F32) * dq - k_run.astype(F32) * dk)
        dg = mm(tri[1], high) + mm(tri[1], low) + boundary
        pre = dg * (-rate_here) * squashed * (1.0 - squashed)
        return dq * jnp.exp(running), dk * jnp.exp(-running), dv, pre

    def put(ref, rows_b, parts):
        dq, dk, dv, pre = parts
        ref[rows_b, 0:DK] = dq.astype(ref.dtype)
        ref[rows_b, DK:2 * DK] = dk.astype(ref.dtype)
        ref[rows_b, 2 * DK:2 * DK + DV] = dv.astype(ref.dtype)
        ref[rows_b, 2 * DK + DV:] = pre.astype(ref.dtype)

    def project(here, weights):
        gate = mm(here, weights(2 * DK + DV, NW))
        return mm(here, weights(0, 2 * DK)), mm(here, weights(2 * DK, 2 * DK + DV)), gate

    def held():
        return made[:, 0:2 * DK], made[:, 2 * DK:2 * DK + DV], made[:, 2 * DK + DV:]

    def hold(parts):
        made[:, 0:2 * DK], made[:, 2 * DK:2 * DK + DV], made[:, 2 * DK + DV:] = parts

    def own_weights(first_col, end_col):
        return w_s[:, first_col:end_col]

    with jax.named_scope("proj"):
        if pairs > 1:
            tok_copy(1).start()
        tok_copy(0).wait()
        hold(project(tok_s[0], own_weights))
        grad_load.wait()

        @pl.loop(1, pairs)
        def _(i):
            @pl.when(i + 1 < pairs)
            def _():
                tok_copy(i + 1).start()

            @pl.when(i == pairs - 1)
            def _():
                if direct is not None:
                    fsw[...] = w_s[group_at(wrap(first + 2), 0, 1), :].astype(F32)
                for m, o in enumerate(near):
                    osend[m] = og_s[chunk(lax.rem(y + o, ny)), :].astype(F32)
                for s in order[:2]:
                    wy_copy(s + 1).wait_recv()
                    start_all(w1_copy, s)
                if direct is not None:
                    fy_copy().start()
                for m, o in enumerate(near[:2]):
                    og_copy(m, o).start()

            tok_copy(i).wait()
            parts = project(tok_s[lax.rem(i, 2)], own_weights)
            absorb(i * 2 - 2, *held(), rate)
            hold(parts)

        for s in order[2:]:
            wy_copy(s + 1).wait_recv()
            start_all(w1_copy, s)
        absorb(blocks - 2, *held(), rate)

    x_chunk = pltpu.make_async_copy(tok_hbm.at[chunk(y)], tok_s.at[0, pl.ds(0, mine)], tok_sem.at[0])
    x_chunk.start()

    def forward_w1(s):
        arrive_all(w1_copy, s)
        if ring > 2:
            start_all(f1_copy, s)

    def start_w2(s, halves=(0, 1)):
        if ring > 2 and 0 in halves:
            arrive_all(f1_copy, s)
        for half in halves:
            for turn in turns:
                w2_copy(s, turn, half).start()

    def arrive_w2(s):
        for half in range(2):
            for turn in turns:
                w2_copy(s, turn, half).wait_recv()

    log_total = carry[0:1, :]
    decay = jnp.exp(log_total)
    dmsg[0, 0:DV, :] = spre[blocks] * decay
    dmsg[1, 0:DV, :] = gpre[blocks]
    for kind in range(2):
        dmsg[kind, DV:DV + 8, :] = jnp.broadcast_to(log_total, (8, DK))

    d_copy = pltpu.make_async_remote_copy(
        dmsg.at[1 - c], dpart, d_sem.at[0], d_sem.at[1], device_id={"seq_2": 1 - c}, device_id_type=MESH)
    with jax.named_scope("d2d"):
        d_copy.start()
        for s in order[:2]:
            forward_w1(s)
        d_copy.wait()

    chip_log = log_total + dpart[DV:DV + 1, :]
    chip = dpart[0:DV, :] + jnp.exp(dpart[DV:DV + 1, :]) * dmsg[c, 0:DV, :]
    for n in range(nz):
        zsend[n, 0:quarter, :] = chip[n * quarter:(n + 1) * quarter, :]
        zsend[n, quarter:quarter + 8, :] = jnp.broadcast_to(chip_log, (8, DK))
    zrecv[z] = zsend[z]
    z_copies = []
    for d in range(1, nz):
        to = lax.rem(z + d, nz)
        z_copies.append(pltpu.make_async_remote_copy(
            zsend.at[to], zrecv.at[z], z_sem.at[0, d - 1], z_sem.at[1, d - 1],
            device_id={"seq_1": to}, device_id_type=MESH))
    for copy in z_copies:
        copy.start()
    with jax.named_scope("w1z"):
        for s in order[2:]:
            forward_w1(s)
        start_w2(order[0])

    with jax.named_scope("zex"):
        for copy in z_copies:
            copy.wait()

    total = jnp.zeros((quarter, DK), F32)
    total_log = jnp.zeros((1, DK), F32)
    for n in range(nz):
        src = c * (nz - 1) + sgn * n
        zexc[src, 0:quarter, :] = total
        zexc[src, quarter:quarter + 8, :] = jnp.broadcast_to(total_log, (8, DK))
        log_here = zrecv[src, quarter:quarter + 1, :]
        total = zrecv[src, 0:quarter, :] + jnp.exp(log_here) * total
        total_log = total_log + log_here
    xsend[0:quarter, :] = total
    xsend[quarter:quarter + 8, :] = jnp.broadcast_to(total_log, (8, DK))

    def x_copy(d):
        to = x + sgn * d
        inside = (to >= 0) & (to < nx)
        return inside, pltpu.make_async_remote_copy(
            xsend, xrecv.at[d - 1], x_sem.at[0, d - 1], x_sem.at[1, d - 1],
            device_id={"seq_0": jnp.where(inside, to, 1 - jnp.minimum(x, 1))}, device_id_type=MESH)

    for d in range(1, nx):
        inside, copy = x_copy(d)
        pl.when(inside)(copy.start)

    for s in order[1:2]:
        start_w2(s, (0,))

    @pl.when(c == 0)
    def _():
        for s in order[1:2]:
            start_w2(s, (1,))

    with jax.named_scope("xex"):
        for d in range(1, nx):
            inside, copy = x_copy(d)
            pl.when(inside)(copy.wait_send)
            source = x - sgn * d
            pl.when((source >= 0) & (source < nx))(copy.wait_recv)

    entering = jnp.zeros((quarter, DK), F32)
    for d in reversed(range(1, nx)):
        entering = xrecv[d - 1, 0:quarter, :] + jnp.exp(xrecv[d - 1, quarter:quarter + 1, :]) * entering
    for n in range(nz):
        fsend[n] = zexc[n, 0:quarter, :] + jnp.exp(zexc[n, quarter:quarter + 1, :]) * entering
    frecv[z] = fsend[z]
    f_copies = []
    for d in range(1, nz):
        to = lax.rem(z + d, nz)
        f_copies.append(pltpu.make_async_remote_copy(
            fsend.at[to], frecv.at[z], f_sem.at[0, d - 1], f_sem.at[1, d - 1],
            device_id={"seq_1": to}, device_id_type=MESH))
    for copy in f_copies:
        copy.start()

    @pl.when(c == 1)
    def _():
        for s in order[1:2]:
            start_w2(s, (1,))

    def forward_w2(s):
        arrive_w2(s)
        if ring > 2 and s != direct:
            start_all(f2_copy, s)

    def group_done(s):
        for n in sorted({0, 1, ring - 1}):
            wd_copy(s, n).start()

    def last_group(s):
        if ring > 2:
            if s == direct:
                fy_copy().wait_recv()
            else:
                arrive_all(f2_copy, s)
            wd_copy(s, 2).start()

    def whole(s):
        for n in range(ring):
            wd_copy(s, n).wait_recv()

    with jax.named_scope("fex"):
        for copy in f_copies:
            copy.wait()
    with jax.named_scope("w2z"):
        forward_w2(order[0])

    entered = frecv[...].reshape(DV, DK)
    psend[...] = dmsg[c, 0:DV, :] + decay * entered
    states[c] = entered
    p_copy = pltpu.make_async_remote_copy(
        psend, states.at[c], p_sem.at[0], p_sem.at[1], device_id={"seq_2": 1 - c}, device_id_type=MESH)
    p_copy.start()
    group_done(order[0])
    with jax.named_scope("pex"):
        p_copy.wait()

    states[1] = states[1] * decay
    for m, o in enumerate(near):
        to = lax.rem(y + o, ny)
        start_log = cs[pl.ds(pl.multiple_of(jnp.maximum(to * mine - 8, 0), 8), 8), :][7:8, :]
        start_log = jnp.where(to > 0, start_log, 0.0)
        ssend[m, 0, 0:DV, :] = (states[0] + spre[to * per_chunk]) * jnp.exp(start_log)
        ssend[m, 1, 0:DV, :] = (states[1] + (gpre[blocks] - gpre[(to + 1) * per_chunk])) * jnp.exp(-start_log)
        ssend[m, 0, DV:DV + 8, :] = jnp.broadcast_to(rate, (8, DK))
        ssend[m, 1, DV:DV + 8, :] = jnp.broadcast_to(rate, (8, DK))

    for m, o in enumerate(near):
        state_copy(m, o).start()

    with jax.named_scope("own"):
        found = [gradients(y * per_chunk + i, states[0], states[1], blocks, rate) for i in range(per_chunk)]
        for i in range(per_chunk):
            gs_hbm[block_rows(y * per_chunk + i), :] = found[i][3] * signal_scale
            put(low, block_rows(i), found[i])
    cols = width

    def mix(grads, weights, last):
        @pl.loop(0, width // cols)
        def _(i):
            at = pl.ds(pl.multiple_of(i * cols, cols), cols)
            term = mm_nt(grads, weights(at))
            if last is None:
                acc[:, at] = term
            elif last:
                out_hbm[:, at] = (acc[:, at] + term).astype(BF16)
            else:
                acc[:, at] = acc[:, at] + term

    def fill(s, m):
        carry[...] = jnp.zeros_like(carry)
        spre[0] = jnp.zeros((DV, DK), F32)
        gpre[0] = jnp.zeros((DV, DK), F32)
        here = tok_s[0, 0:mine, :]
        qk, val, gate = project(here, lambda first_col, end_col: wl[s, :, first_col:end_col].astype(BF16))
        if m == min(1, len(near) - 1):
            with jax.named_scope("w2c"):
                for later in order[2:]:
                    forward_w2(later)
                    group_done(later)
        with jax.named_scope(f"ogw{m}"):
            og_copy(m, near[m]).wait_recv()
        with jax.named_scope(f"stw{m}"):
            state_copy(m, near[m]).wait_recv()
        og_s[0:mine, :] = orecv[m].astype(BF16)
        rate_here = srecv[m, 0, DV:DV + 1, :]
        absorb(0, qk, val, gate, rate_here)
        found = [gradients(i, srecv[m, 0, 0:DV, :], srecv[m, 1, 0:DV, :], per_chunk, rate_here)
                for i in range(per_chunk)]
        for i in range(per_chunk):
            put(low, block_rows(i), found[i])

    with jax.named_scope("mix_own"):
        mix(low[...], lambda at: w_s[at, :], None)
    with jax.named_scope("w2a"):
        for s in order[1:2]:
            forward_w2(s)
            group_done(s)
        for s in order[2:]:
            start_w2(s)
    with jax.named_scope("signals"):
        @pl.loop(1, ny)
        def _(n):
            @pl.when(n == ny - 1)
            def _():
                last_group(order[0])

            first_b = lax.rem(y + n, ny) * per_chunk
            found = [gradients(first_b + i, states[0], states[1], blocks, rate)[3] for i in range(per_chunk)]
            for i in range(per_chunk):
                gs_hbm[block_rows(first_b + i), :] = found[i] * signal_scale

    for m, o in enumerate(near):
        if m >= 2:
            og_copy(m, o).start()
    if direct is not None:
        last_group(direct)
    x_chunk.wait()
    for m, o in enumerate(near):
        s = o - 1
        with jax.named_scope(f"whole{m}"):
            if m > 1 and s != direct:
                last_group(s)
            whole(s)
        with jax.named_scope(f"fill{m}"):
            fill(s, m)
        if m == 0:
            for later in order[1:2]:
                last_group(later)
        with jax.named_scope(f"mix{m}"):
            mix(low[...], lambda at: wl[s, at, :].astype(BF16), s == order[-1])
    with jax.named_scope("end"):
        for s in order:
            wy_copy(s + 1).wait_send()
            for turn in turns:
                w1_copy(s, turn).wait_send()
                w2_copy(s, turn, 0).wait_send()
                w2_copy(s, turn, 1).wait_send()
                if ring > 2:
                    f1_copy(s, turn).wait_send()
                    if s != direct:
                        f2_copy(s, turn).wait_send()
            for n in range(ring):
                wd_copy(s, n).wait_send()
        if direct is not None:
            fy_copy().wait_send()
        for m, o in enumerate(near):
            og_copy(m, o).wait_send()
            state_copy(m, o).wait_send()


def per_device(dims, tokens, w_query, w_key, w_value, w_gate, gate_rate, out_grad):
    nx, nz, ny = dims
    rows, width = tokens.shape
    blocks = rows // BT
    mine = rows // ny
    quarter = DV // nz
    whole_tokens = rows * nx * nz * 2
    signal_scale = 4.0 * math.sqrt(whole_tokens * DK / DV)

    count_near = ny - 1
    any_spec = pl.BlockSpec(memory_space=pl.ANY)
    vmem_spec = pl.BlockSpec(memory_space=pltpu.VMEM)
    dma = pltpu.SemaphoreType.DMA
    mixed, signal = pl.pallas_call(
        functools.partial(body, (nx, nz, ny, rows, width, blocks), signal_scale),
        out_shape=(
            pltpu.VMEM((mine, width), BF16),
            pltpu.VMEM((rows, DK), F32),
        ),
        in_specs=[any_spec] * 5 + [vmem_spec, any_spec],
        out_specs=(vmem_spec, vmem_spec),
        scratch_shapes=[
            pltpu.VMEM((width, NW), BF16),
            pltpu.VMEM((2, 2 * BT, width), BF16),
            pltpu.VMEM((rows, DV), BF16),
            pltpu.VMEM((rows, DK), BF16),
            pltpu.VMEM((rows, DK), BF16),
            pltpu.VMEM((rows, DV), BF16),
            pltpu.VMEM((rows, DK), F32),
            pltpu.VMEM((rows, DK), F32),
            pltpu.VMEM((2, BT, BT), BF16),
            pltpu.VMEM((8, DK), F32),
            pltpu.VMEM((blocks + 1, DV, DK), F32),
            pltpu.VMEM((blocks + 1, DV, DK), F32),
            pltpu.VMEM((2, DV + 8, DK), F32),
            pltpu.VMEM((DV + 8, DK), F32),
            pltpu.VMEM((nz, quarter + 8, DK), F32),
            pltpu.VMEM((nz, quarter + 8, DK), F32),
            pltpu.VMEM((nz, quarter + 8, DK), F32),
            pltpu.VMEM((quarter + 8, DK), F32),
            pltpu.VMEM((nx - 1, quarter + 8, DK), F32),
            pltpu.VMEM((nz, quarter, DK), F32),
            pltpu.VMEM((nz, quarter, DK), F32),
            pltpu.VMEM((DV, DK), F32),
            pltpu.VMEM((2, DV, DK), F32),
            pltpu.VMEM((mine, width), F32),
            pltpu.VMEM((width // (nx * nz * 2), NW), F32),
            pltpu.VMEM((ny - 1, width, NW), F32),
            pltpu.VMEM((mine, NW), BF16),
            pltpu.VMEM((2 * BT, NW), F32),
            pltpu.VMEM((width // (2 * nx), NW), F32),
            pltpu.VMEM((count_near, mine, DV), F32),
            pltpu.VMEM((count_near, mine, DV), F32),
            pltpu.VMEM((count_near, 2, DV + 8, DK), F32),
            pltpu.VMEM((count_near, 2, DV + 8, DK), F32),
            dma((5,)),
            dma((2,)),
            dma((2,)),
            dma((2, nz - 1)),
            dma((2, nx - 1)),
            dma((2, nz - 1)),
            dma((2,)),
            dma((2,)),
            dma((2, ny - 1)),
            dma((2, ny - 1, 2)),
            dma((2, ny - 1, 2)),
            dma((2, ny - 1, 2, 2)),
            dma((2, ny - 1, 2)),
            dma((2, ny - 1, nx)),
            dma((2, count_near)),
            dma((2, count_near)),
            dma((2,)),
        ],
        compiler_params=pltpu.CompilerParams(
            collective_id=0, has_side_effects=True, vmem_limit_bytes=56 * 2**20),
        cost_estimate=pl.CostEstimate(
            flops=40_000_000_000, bytes_accessed=30_000_000, transcendentals=1_000_000),
    )(tokens, w_query, w_key, w_value, w_gate, gate_rate.reshape(1, DK), out_grad)

    return mixed, signal


def solution(mesh, shape=(4, 4)):
    nx, nz = shape
    ny = mesh.shape["tp"]
    torus = Mesh(mesh.devices.reshape(nx, nz, 2, ny), SEQ_TP)
    placed = (
        P(SEQ, None),
        P(None, "tp"),
        P(None, "tp"),
        P(None, "tp"),
        P(None, "tp"),
        P("tp"),
        P(SEQ, "tp"),
    )
    return jax.shard_map(
        functools.partial(per_device, (nx, nz, ny)),
        mesh=torus,
        in_specs=placed,
        out_specs=(P(SEQ_TP, None), P(SEQ, "tp")),
        check_vma=False,
    )
```
